256 devices in a mesh: row: 32 (over z, y), col: 8 (over x, core).
Axes of the slice: x: 4, y: 4, z: 8, core: 2. Of those that a mesh axis runs over, the one named last changes fastest.
Arguments:
- weights: float32 [2, 1, 8192, 4, 2048], P(None, None, 'row', None, 'col'), may hold values from -6 to 6
Outputs:
- trailing: float32 [2, 1, 8192, 4, 2048], P(None, None, 'row', None, 'col')
- diagonal: float32 [2, 12], replicated
- superdiag: float32 [2, 12], replicated
The draws below stay inside these ranges and needn't reach their ends.
All inputs are finite; a program needn't handle non-finite values.
Results may differ from the reference program's by a relative error of at most 0.0003.
Values sent between devices are 32-bit elements; how exact they have to be, the bound alone decides.
No kernel may reach another device: no remote copies, remote signals or barrier semaphores. Data moves between devices by JAX's collectives and lax.ppermute only.
A program may use at most 64 MiB of HBM per device.

```python
import jax
import jax.numpy as jnp
from jax import lax

N = 8192
TILE = 256
STEPS = 6
PANELS = 2
MATS = 2
RCYC = 1
CCYC = 4
N_ROW = 32
N_COL = 8


def level_of(rng, shape, split, low, top_value):
    loudness = 1.0
    for position, shards_of in split:
        draws = jax.random.uniform(jax.random.fold_in(jax.random.fold_in(rng, 6), position), (shards_of,), jnp.float32, low / len(split), top_value / len(split))
        loudness = loudness * jnp.repeat(jnp.exp(draws), shape[position] // shards_of).reshape((-1,) + (1,) * (len(shape) - 1 - position))
    return loudness


def scatter_about(own_key, dims, width, limit, pieces=(), kind=jnp.bfloat16):
    values = jax.random.normal(own_key, dims, jnp.float32) * width
    if len(pieces) > 0:
        values = level_of(own_key, dims, pieces, -0.22, 0.18) * values
    return jnp.clip(values, min=-limit, max=limit).astype(kind)


def setup_inputs(seed: int = 0) -> dict:
    key_list = jax.random.split(jax.random.key(seed), 2)
    return {
        "weights": scatter_about(key_list[0], (MATS, RCYC, N_ROW * TILE, CCYC, N_COL * TILE), 1.0, 6.0, ((2, 32), (4, 8)), jnp.float32),
    }


def contract(form, left, right):
    return jnp.einsum(form, left, right, precision=lax.Precision.HIGHEST)

def reflect(leading, squares):
    length = jnp.sqrt(squares)
    divisor = jnp.maximum(leading + length, 1.0)
    factor = (leading + length) / jnp.maximum(length, 1.0)
    return (divisor, factor, -length)

def reference(weights):
    mats = weights.reshape(MATS, N, N)
    global_ids = jnp.arange(N, dtype=jnp.int32)
    diag_list = []
    super_list = []
    for panel_at in range(PANELS):
        first_at = panel_at * STEPS
        col_refl = jnp.zeros((MATS, STEPS, N), jnp.float32)
        col_aux = jnp.zeros((MATS, STEPS, N), jnp.float32)
        row_aux = jnp.zeros((MATS, STEPS, N), jnp.float32)
        row_refl = jnp.zeros((MATS, STEPS, N), jnp.float32)
        for step_at in range(STEPS):
            pivot = first_at + step_at
            col_piece = mats[:, :, pivot] - contract('mp,mpr->mr', row_aux[:, :, pivot], col_refl) - contract('mp,mpr->mr', row_refl[:, :, pivot], col_aux)
            col_piece = jnp.where(global_ids >= pivot, col_piece, 0.0)
            divisor, factor, bidiag = reflect(col_piece[:, pivot], lax.optimization_barrier(jnp.sum(col_piece * col_piece, axis=1)))
            col_vec = jnp.where(global_ids == pivot, 1.0, col_piece / divisor[:, None])
            col_refl = col_refl.at[:, step_at].set(col_vec)
            weighs_one = contract('mpr,mr->mp', col_refl, col_vec)
            weighs_two = contract('mpr,mr->mp', col_aux, col_vec)
            col_img = factor[:, None] * (contract('mrc,mr->mc', mats, col_vec) - contract('mp,mpc->mc', weighs_one, row_aux) - contract('mp,mpc->mc', weighs_two, row_refl))
            col_img = jnp.where(global_ids > pivot, col_img, 0.0)
            row_aux = row_aux.at[:, step_at].set(col_img)
            row_piece = mats[:, pivot, :] - contract('mp,mpc->mc', col_refl[:, :, pivot], row_aux) - contract('mp,mpc->mc', col_aux[:, :, pivot], row_refl)
            row_piece = jnp.where(global_ids > pivot, row_piece, 0.0)
            divisor2, factor2, bidiag2 = reflect(row_piece[:, pivot + 1], lax.optimization_barrier(jnp.sum(row_piece * row_piece, axis=1)))
            row_vec = jnp.where(global_ids == pivot + 1, 1.0, row_piece / divisor2[:, None])
            row_refl = row_refl.at[:, step_at].set(row_vec)
            dots_one = contract('mpc,mc->mp', row_aux, row_vec)
            dots_two = contract('mpc,mc->mp', row_refl, row_vec)
            row_img = factor2[:, None] * (contract('mrc,mc->mr', mats, row_vec) - contract('mp,mpr->mr', dots_one, col_refl) - contract('mp,mpr->mr', dots_two, col_aux))
            row_img = jnp.where(global_ids > pivot, row_img, 0.0)
            col_aux = col_aux.at[:, step_at].set(row_img)
            diag_list.append(bidiag)
            super_list.append(bidiag2)
        mats = mats - contract('mpr,mpc->mrc', col_refl, row_aux) - contract('mpr,mpc->mrc', col_aux, row_refl)
    done = PANELS * STEPS
    inside = (global_ids[:, None] >= done) & (global_ids[None, :] >= done)
    trailing = jnp.where(inside[None], mats, 0.0).reshape(weights.shape)
    return (trailing, jnp.stack(diag_list, axis=1), jnp.stack(super_list, axis=1))
```

```python
import functools

import jax
import jax.numpy as jnp
from jax import lax
from jax.experimental import pallas as pl
from jax.experimental.pallas import tpu as pltpu
from jax.sharding import PartitionSpec as P

TOTAL = 12
SLOTS = 16
LANES = 128
AT_SQUARES, AT_LEAD, AT_SECOND, AT_PICK, AT_PICK2 = 32, 33, 16, 64, 80
VMEM = pl.BlockSpec(memory_space=pltpu.VMEM)
F32 = jnp.float32


def spread(row):
    return jnp.transpose(jnp.broadcast_to(row, (LANES, LANES)))


def gather_lanes(rows):
    return jnp.sum(jnp.transpose(rows), axis=0, keepdims=True)


def total(x):
    return jnp.sum(x, axis=0, keepdims=True)


def wide(x, n):
    return jnp.concatenate([x] * n, axis=1)


def fold(x):
    return sum(x[:, at : at + LANES] for at in range(0, x.shape[1], LANES))


def dots_row(first, second, squares, lead, pick, pick2):
    at = lax.broadcasted_iota(jnp.int32, (SLOTS, LANES), 0)
    pair = jnp.where(at == 0, squares, jnp.where(at == 1, lead, 0.0))
    none = jnp.zeros((SLOTS, LANES), F32)
    return gather_lanes(jnp.concatenate([first, second, pair, none, pick, pick2, none, none], axis=0))


def reflect(dots):
    lead = dots[AT_LEAD : AT_LEAD + 1]
    length = jnp.sqrt(dots[AT_SQUARES : AT_SQUARES + 1])
    divisor = jnp.maximum(lead + length, 1.0)
    factor = (lead + length) / jnp.maximum(length, 1.0)
    return divisor, factor, 1.0 - lead / divisor, -length


def slot(ref, at):
    return ref.at[at : at + 1]


def tiles(ref):
    return [slice(at, at + LANES) for at in range(0, ref.shape[1], LANES)]


def finish_row_side(step, sums, r_ref, gr_ref, gc_ref, cols_ref, v_ref, x_ref, u_ref, sd_ref):
    rows = gr_ref.shape[1]
    dots = spread(sums[:, rows:])
    divisor, factor, remain, bidiag = reflect(dots)
    pick, pick2 = dots[AT_PICK : AT_PICK + SLOTS], dots[AT_PICK2 : AT_PICK2 + SLOTS]
    one = dots[:SLOTS] / divisor + pick * remain
    two = dots[AT_SECOND : AT_SECOND + SLOTS] / divisor + pick2 * remain
    n = rows // LANES
    col = cols_ref[step : step + 1]
    v, x = v_ref[...], x_ref[...]
    image = wide(factor, n) * (
        sums[:, :rows] / wide(divisor, n)
        + col * wide(remain, n)
        - total(wide(one, n) * v + wide(two, n) * x)
    )
    image = jnp.where(gr_ref[...] >= step, image, 0.0)
    column = col - total(wide(pick, n) * v + wide(pick2, n) * x) - image
    x_ref[step - 1 : step, :] = image
    sd_ref[step - 1 : step, :] = bidiag
    for ts in tiles(r_ref):
        u_ref[step - 1 : step, ts] = jnp.where(gc_ref[:, ts] == step, 1.0, r_ref[:, ts] / divisor)
    return jnp.where(gr_ref[...] >= step, column, 0.0)


def send_row(step, column, gr_ref, own_ref, oth_ref, v_ref, x_ref, msg_ref, c_ref, extra=None):
    rows = gr_ref.shape[1]
    c_ref[...] = column
    spread_c = jnp.transpose(jnp.broadcast_to(column, (LANES, rows)))
    parts = []
    for ref in (own_ref, oth_ref):
        for ts in tiles(ref):
            parts.append(total(ref[:, ts] * spread_c))
    hit = gr_ref[...] == step
    lead = fold(jnp.where(hit, column, 0.0))
    squares = fold(column * column)
    if v_ref is None:
        none = jnp.zeros((SLOTS, LANES), F32)
        parts.append(dots_row(none, none, squares, lead, none, none))
    else:
        v, x = v_ref[...], x_ref[...]
        parts.append(
            dots_row(
                fold(v * column),
                fold(x * column),
                squares,
                lead,
                fold(jnp.where(hit, v, 0.0)),
                fold(jnp.where(hit, x, 0.0)),
            )
        )
    if extra is not None:
        parts.append(extra)
    message = jnp.concatenate(parts, axis=1)
    for peer in range(msg_ref.shape[0]):
        msg_ref[peer] = message


def carry(before, after):
    for old, new in zip(before, after):
        new[...] = old[...]


def first_kernel(gr_ref, cols_ref, scat_ref, own_ref, oth_ref, msg_ref, c_ref, *state):
    for ref in state:
        ref[...] = jnp.zeros_like(ref)
    send_row(0, cols_ref[0:1], gr_ref, own_ref, oth_ref, None, None, msg_ref, c_ref, scat_ref[0])


def column_kernel(
    step, a_ref, b_ref, r_ref, gr_ref, gc_ref, cols_ref, own_ref, oth_ref, v_ref,
    x_in, u_in, sd_in, msg_ref, c_ref, x_ref, u_ref, sd_ref,
):
    carry((x_in, u_in, sd_in), (x_ref, u_ref, sd_ref))
    sums = a_ref[...] + b_ref[...]
    column = finish_row_side(
        step, sums, r_ref, gr_ref, gc_ref, cols_ref, v_ref, x_ref, u_ref, sd_ref
    )
    send_row(step, column, gr_ref, own_ref, oth_ref, v_ref, x_ref, msg_ref, c_ref)


def last_kernel(
    a_ref, b_ref, r_ref, gr_ref, gc_ref, cols_ref, v_ref, y_ref, dg_ref,
    x_in, u_in, sd_in, own_ref, oth_ref, x_ref, u_ref, sd_ref,
):
    carry((x_in, u_in, sd_in), (x_ref, u_ref, sd_ref))
    sums = a_ref[...] + b_ref[...]
    finish_row_side(TOTAL, sums, r_ref, gr_ref, gc_ref, cols_ref, v_ref, x_ref, u_ref, sd_ref)
    rows, half = gr_ref.shape[1], gc_ref.shape[1] // 2
    for ref, begin in ((own_ref, 0), (oth_ref, half)):
        ref[:SLOTS, :rows] = v_ref[...]
        ref[SLOTS:, :rows] = x_ref[...]
        ref[:SLOTS, rows : rows + half] = y_ref[:, begin : begin + half]
        ref[SLOTS:, rows : rows + half] = u_ref[:, begin : begin + half]
        ref[:SLOTS, rows + half :] = dg_ref[...]
        ref[SLOTS:, rows + half :] = sd_ref[...]


def row_kernel(
    step, recv_ref, c_ref, gr_ref, gc_ref, *refs,
):
    if step == 0:
        own_ref, oth_ref, u_ref, v_in, y_in, dg_in, msg_ref, r_ref, v_ref, y_ref, dg_ref, piv_ref = refs
    else:
        piv_ref, own_ref, oth_ref, u_ref, v_in, y_in, dg_in, msg_ref, r_ref, v_ref, y_ref, dg_ref = refs
    carry((v_in, y_in, dg_in), (v_ref, y_ref, dg_ref))
    cols = gc_ref.shape[1]
    summed = recv_ref[0, :, : cols + LANES]
    for peer in range(1, recv_ref.shape[0]):
        summed = summed + recv_ref[peer, :, : cols + LANES]
    if step == 0:
        piece = recv_ref.shape[2] - cols - LANES
        piv_ref[TOTAL:, :] = jnp.zeros((SLOTS - TOTAL, cols), F32)
        for peer in range(recv_ref.shape[0]):
            for at in range(0, piece, LANES):
                flat = peer * piece + at
                row, begin = flat // cols, flat % cols
                piv_ref[row : row + 1, begin : begin + LANES] = recv_ref[
                    peer, :, cols + LANES + at : cols + 2 * LANES + at
                ]
    dots = spread(summed[:, cols:])
    divisor, factor, remain, bidiag = reflect(dots)
    pick, pick2 = dots[AT_PICK : AT_PICK + SLOTS], dots[AT_PICK2 : AT_PICK2 + SLOTS]
    one = dots[:SLOTS] / divisor + pick * remain
    two = dots[AT_SECOND : AT_SECOND + SLOTS] / divisor + pick2 * remain
    dg_ref[step : step + 1, :] = bidiag
    n = gr_ref.shape[1] // LANES
    v_ref[step : step + 1, :] = jnp.where(gr_ref[...] == step, 1.0, c_ref[...] / wide(divisor, n))
    at_slot = lax.broadcasted_iota(jnp.int32, (SLOTS, LANES), 0) == step
    image = jnp.zeros((own_ref.shape[0], LANES), F32)
    first = second = pick_y = pick_u = jnp.zeros((SLOTS, LANES), F32)
    squares = lead = jnp.zeros((1, LANES), F32)
    half = cols // 2
    for begin in range(0, cols, LANES):
        ts = slice(begin, begin + LANES)
        y_t, u_t, piv_t, gc_t = y_ref[:, ts], u_ref[:, ts], piv_ref[step : step + 1, ts], gc_ref[:, ts]
        y = factor * (summed[:, ts] / divisor + piv_t * remain - total(one * y_t + two * u_t))
        y = jnp.where(gc_t > step, y, 0.0)
        r = piv_t - total(pick * y_t + pick2 * u_t) - y
        r = jnp.where(gc_t > step, r, 0.0)
        y_ref[step : step + 1, ts] = y
        r_ref[:, ts] = r
        y_t = jnp.where(at_slot, y, y_t)
        first, second, squares = first + y_t * r, second + u_t * r, squares + r * r
        if begin % half == 0:
            hit = gc_t == step + 1
            lead = lead + jnp.where(hit, r, 0.0)
            pick_y = pick_y + jnp.where(hit, y_t, 0.0)
            pick_u = pick_u + jnp.where(hit, u_t, 0.0)
        block = own_ref[:, ts] if begin < half else oth_ref[:, begin - half : begin - half + LANES]
        image = image + block * r
    msg_ref[...] = jnp.concatenate(
        [gather_lanes(image), dots_row(first, second, squares, lead, pick_y, pick_u)], axis=1
    )


def call(kernel, name, ins, outs):
    return pl.pallas_call(
        kernel,
        name=name,
        out_shape=[pltpu.VMEM(s, F32) for s in outs],
        in_specs=[VMEM] * len(ins),
        out_specs=[VMEM] * len(outs),
    )(*(pltpu.with_memory_space_constraint(x, pltpu.VMEM) for x in ins))


def per_device(weights):
    batch_n, row_cycles, tile_len, col_cycles, _ = weights.shape
    rows, cols = row_cycles * tile_len, col_cycles * tile_len
    w = weights.reshape(batch_n, rows, cols)
    row_devices, col_devices = lax.axis_size("row"), lax.axis_size("col")
    row_place, col_place = lax.axis_index("row"), lax.axis_index("col")
    core, chip = col_place % 2, col_place // 2
    chips = col_devices // 2
    everyone = range(col_devices)
    swap = [(i, i ^ 1) for i in everyone]
    near = [(i, i ^ 2) for i in everyone]
    far = [(i, 2 * (chips - 1 - i // 2) + i % 2) for i in everyone]

    col_ids = jnp.arange(cols, dtype=jnp.int32)

    def global_cols(place):
        return col_ids // tile_len * (col_devices * tile_len) + place * tile_len + col_ids % tile_len

    gcol = global_cols(col_place)
    gc = jnp.concatenate([gcol, global_cols(col_place ^ 1)])[None]
    grow = row_place * tile_len + jnp.arange(rows, dtype=jnp.int32)
    gr = grow[None]

    own = jnp.where(core == 0, w[0], w[1])
    oth = lax.ppermute(jnp.where(core == 0, w[1], w[0]), "col", swap)

    both = 2 * cols
    piece = TOTAL * both // row_devices
    scat = jnp.concatenate([own[:TOTAL], oth[:TOTAL]], axis=1).reshape(row_devices, 1, piece)
    scat = lax.all_to_all(scat, "row", split_axis=0, concat_axis=0, tiled=True)
    slab = jnp.where(core == 0, own[:, :SLOTS], oth[:, :SLOTS]).T
    slab = jnp.where(chip == 0, slab, 0.0)
    slab = slab + lax.ppermute(slab, "col", [(0, 2), (1, 3)])
    first_cols = slab + lax.ppermute(slab, "col", [(0, 6), (1, 7), (2, 4), (3, 5)])

    vec_r, vec_c, flag = (SLOTS, rows), (SLOTS, both), (SLOTS, LANES)
    msg = (row_devices, 1, both + LANES)
    msg_long = (row_devices, 1, both + LANES + piece)
    out = call(
        first_kernel,
        "first",
        (gr, first_cols, scat, own, oth),
        (msg_long, (1, rows), vec_r, vec_r, vec_c, vec_c, flag, flag),
    )
    message, column, v, x, y, u, dg, sd = out
    pivots = None
    for step in range(TOTAL):
        recv = lax.all_to_all(message, "row", split_axis=0, concat_axis=0, tiled=True)
        lead_in = (recv, column, gr, gc)
        state = (own, oth, u, v, y, dg)
        outs = ((1, rows + LANES), (1, both), vec_r, vec_c, flag)
        kernel = functools.partial(row_kernel, step)
        if step == 0:
            ins, outs = lead_in + state, outs + (vec_c,)
            message, r, v, y, dg, pivots = call(kernel, "row_step", ins, outs)
        else:
            ins = lead_in + (pivots,) + state
            message, r, v, y, dg = call(kernel, "row_step", ins, outs)
        part = message + lax.ppermute(message, "col", near)
        rest = lax.ppermute(part, "col", far)
        if step + 1 < TOTAL:
            ins = (part, rest, r, gr, gc, first_cols, own, oth, v, x, u, sd)
            message, column, x, u, sd = call(
                functools.partial(column_kernel, step + 1),
                "column_step",
                ins,
                (msg, (1, rows), vec_r, vec_c, flag),
            )
    ins = (part, rest, r, gr, gc, first_cols, v, y, dg, x, u, sd)
    packed = (2 * SLOTS, rows + cols + LANES)
    mine, theirs, _, _, _ = call(last_kernel, "last", ins, (packed, packed, vec_r, vec_c, flag))
    theirs = lax.ppermute(theirs, "col", swap)
    packs = jnp.stack(
        [jnp.where(core == 0, mine, theirs), jnp.where(core == 0, theirs, mine)]
    )
    change = jnp.einsum(
        "mpr,mpc->mrc",
        packs[:, :, :rows],
        packs[:, :, rows : rows + cols],
        precision=lax.Precision.HIGHEST,
    )
    inside = (grow[:, None] >= TOTAL) & (gcol[None, :] >= TOTAL)
    trailing = jnp.where(inside[None], w - change, 0.0).reshape(weights.shape)
    ends = packs[:, :, rows + cols]
    return trailing, ends[:, :TOTAL], ends[:, SLOTS : SLOTS + TOTAL]


def solution(mesh):
    placed = P(None, None, "row", None, "col")
    return jax.shard_map(
        per_device,
        mesh=mesh,
        in_specs=(placed,),
        out_specs=(placed, P(), P()),
        check_vma=False,
    )
```

```python
import functools

import jax
import jax.numpy as jnp
from jax import lax
from jax.experimental import pallas as pl
from jax.experimental.pallas import tpu as pltpu
from jax.sharding import PartitionSpec as P

TOTAL = 12
SLOTS = 16
LANES = 128
AT_SQUARES, AT_LEAD, AT_SECOND, AT_PICK, AT_PICK2 = 32, 33, 16, 64, 80
VMEM = pl.BlockSpec(memory_space=pltpu.VMEM)
F32 = jnp.float32


def spread(row):
    return jnp.transpose(jnp.broadcast_to(row, (LANES, LANES)))


def gather_lanes(rows):
    return jnp.sum(jnp.transpose(rows), axis=0, keepdims=True)


def total(x):
    return jnp.sum(x, axis=0, keepdims=True)


def wide(x, n):
    return jnp.concatenate([x] * n, axis=1)


def fold(x):
    return sum(x[:, at : at + LANES] for at in range(0, x.shape[1], LANES))


def dots_row(first, second, squares, lead, pick, pick2):
    at = lax.broadcasted_iota(jnp.int32, (SLOTS, LANES), 0)
    pair = jnp.where(at == 0, squares, jnp.where(at == 1, lead, 0.0))
    none = jnp.zeros((SLOTS, LANES), F32)
    return gather_lanes(jnp.concatenate([first, second, pair, none, pick, pick2, none, none], axis=0))


def reflect(dots):
    lead = dots[AT_LEAD : AT_LEAD + 1]
    length = jnp.sqrt(dots[AT_SQUARES : AT_SQUARES + 1])
    divisor = jnp.maximum(lead + length, 1.0)
    factor = (lead + length) / jnp.maximum(length, 1.0)
    return divisor, factor, 1.0 - lead / divisor, -length


def slot(ref, at):
    return ref.at[at : at + 1]


def tiles(ref):
    return [slice(at, at + LANES) for at in range(0, ref.shape[1], LANES)]


def finish_row_side(step, sums, r_ref, gr_ref, gc_ref, cols_ref, v_ref, x_ref, u_ref, sd_ref):
    rows = gr_ref.shape[1]
    dots = spread(sums[:, rows:])
    divisor, factor, remain, bidiag = reflect(dots)
    pick, pick2 = dots[AT_PICK : AT_PICK + SLOTS], dots[AT_PICK2 : AT_PICK2 + SLOTS]
    one = dots[:SLOTS] / divisor + pick * remain
    two = dots[AT_SECOND : AT_SECOND + SLOTS] / divisor + pick2 * remain
    n = rows // LANES
    col = cols_ref[step : step + 1]
    v, x = v_ref[...], x_ref[...]
    image = wide(factor, n) * (
        sums[:, :rows] / wide(divisor, n)
        + col * wide(remain, n)
        - total(wide(one, n) * v + wide(two, n) * x)
    )
    image = jnp.where(gr_ref[...] >= step, image, 0.0)
    column = col - total(wide(pick, n) * v + wide(pick2, n) * x) - image
    x_ref[step - 1 : step, :] = image
    sd_ref[step - 1 : step, :] = bidiag
    for ts in tiles(r_ref):
        u_ref[step - 1 : step, ts] = jnp.where(gc_ref[:, ts] == step, 1.0, r_ref[:, ts] / divisor)
    return jnp.where(gr_ref[...] >= step, column, 0.0)


def send_row(step, column, gr_ref, own_ref, oth_ref, v_ref, x_ref, msg_ref, c_ref, extra=None):
    rows = gr_ref.shape[1]
    c_ref[...] = column
    spread_c = jnp.transpose(jnp.broadcast_to(column, (LANES, rows)))
    parts = []
    for ref in (own_ref, oth_ref):
        for ts in tiles(ref):
            parts.append(total(ref[:, ts] * spread_c))
    hit = gr_ref[...] == step
    lead = fold(jnp.where(hit, column, 0.0))
    squares = fold(column * column)
    if v_ref is None:
        none = jnp.zeros((SLOTS, LANES), F32)
        parts.append(dots_row(none, none, squares, lead, none, none))
    else:
        v, x = v_ref[...], x_ref[...]
        parts.append(
            dots_row(
                fold(v * column),
                fold(x * column),
                squares,
                lead,
                fold(jnp.where(hit, v, 0.0)),
                fold(jnp.where(hit, x, 0.0)),
            )
        )
    if extra is not None:
        parts.append(extra)
    message = jnp.concatenate(parts, axis=1)
    for peer in range(msg_ref.shape[0]):
        msg_ref[peer] = message


def carry(before, after):
    for old, new in zip(before, after):
        new[...] = old[...]


def open_kernel(core_ref, chip_ref, own_ref, oth_ref, slab_ref):
    slab = jnp.where(core_ref[...] == 0, own_ref[:, :LANES], oth_ref[:, :LANES])
    slab = jnp.transpose(slab)[:SLOTS]
    n = slab.shape[1] // LANES
    slab_ref[...] = jnp.where(wide(chip_ref[...], n) == 0, slab, 0.0)


def first_kernel(gr_ref, cols_ref, own_ref, oth_ref, msg_ref, c_ref, *state):
    for ref in state:
        ref[...] = jnp.zeros_like(ref)
    half = own_ref.shape[1]
    row = jnp.concatenate([own_ref[0:1], oth_ref[0:1]], axis=1)
    base = 4 * half + LANES
    send_row(
        0, cols_ref[0:1], gr_ref, own_ref, oth_ref, None, None, msg_ref.at[:, :, :base], c_ref, row
    )
    piece = msg_ref.shape[2] - base
    for peer in range(msg_ref.shape[0]):
        for at in range(0, piece, LANES):
            row, begin = divmod(peer * piece + at, 2 * half)
            ref = own_ref if begin < half else oth_ref
            begin %= half
            msg_ref[peer, :, base + at : base + at + LANES] = ref[row : row + 1, begin : begin + LANES]


def column_kernel(
    step, a_ref, b_ref, r_ref, gr_ref, gc_ref, cols_ref, own_ref, oth_ref, v_ref,
    x_in, u_in, sd_in, *refs,
):
    piece_ref = refs[0] if step == 1 else None
    msg_ref, c_ref, x_ref, u_ref, sd_ref = refs[-5:]
    carry((x_in, u_in, sd_in), (x_ref, u_ref, sd_ref))
    sums = a_ref[...] + b_ref[...]
    column = finish_row_side(
        step, sums, r_ref, gr_ref, gc_ref, cols_ref, v_ref, x_ref, u_ref, sd_ref
    )
    extra = None if piece_ref is None else piece_ref[...]
    send_row(step, column, gr_ref, own_ref, oth_ref, v_ref, x_ref, msg_ref, c_ref, extra)


def last_kernel(
    a_ref, b_ref, r_ref, gr_ref, gc_ref, cols_ref, v_ref, y_ref, dg_ref,
    x_in, u_in, sd_in, own_ref, oth_ref, x_ref, u_ref, sd_ref,
):
    carry((x_in, u_in, sd_in), (x_ref, u_ref, sd_ref))
    sums = a_ref[...] + b_ref[...]
    finish_row_side(TOTAL, sums, r_ref, gr_ref, gc_ref, cols_ref, v_ref, x_ref, u_ref, sd_ref)
    rows, half = gr_ref.shape[1], gc_ref.shape[1] // 2
    for ref, begin in ((own_ref, 0), (oth_ref, half)):
        ref[:SLOTS, :rows] = v_ref[...]
        ref[SLOTS:, :rows] = x_ref[...]
        ref[:SLOTS, rows : rows + half] = y_ref[:, begin : begin + half]
        ref[SLOTS:, rows : rows + half] = u_ref[:, begin : begin + half]
        ref[:SLOTS, rows + half :] = dg_ref[...]
        ref[SLOTS:, rows + half :] = sd_ref[...]


def row_kernel(
    step, recv_ref, c_ref, gr_ref, gc_ref, *refs,
):
    own_ref, oth_ref, u_ref, v_in, y_in, dg_in = refs[:6]
    if step == 0:
        msg_ref, r_ref, v_ref, y_ref, dg_ref, piece_ref = refs[6:]
    elif step == 1:
        msg_ref, r_ref, v_ref, y_ref, dg_ref, piv_ref = refs[6:]
    else:
        piv_ref, msg_ref, r_ref, v_ref, y_ref, dg_ref = refs[6:]
    carry((v_in, y_in, dg_in), (v_ref, y_ref, dg_ref))
    cols = gc_ref.shape[1]
    base = cols + LANES
    summed = recv_ref[0, :, :base]
    for peer in range(1, recv_ref.shape[0]):
        summed = summed + recv_ref[peer, :, :base]
    if step == 0:
        pivot = recv_ref[0, :, base : base + cols]
        piece_ref[...] = recv_ref[0, :, base + cols :]
    else:
        if step == 1:
            piece = recv_ref.shape[2] - base
            piv_ref[TOTAL:, :] = jnp.zeros((SLOTS - TOTAL, cols), F32)
            for peer in range(recv_ref.shape[0]):
                for at in range(0, piece, LANES):
                    row, begin = divmod(peer * piece + at, cols)
                    part = recv_ref[peer, :, base + at : base + at + LANES]
                    piv_ref[row : row + 1, begin : begin + LANES] = part
        pivot = piv_ref[step : step + 1]
    dots = spread(summed[:, cols:])
    divisor, factor, remain, bidiag = reflect(dots)
    pick, pick2 = dots[AT_PICK : AT_PICK + SLOTS], dots[AT_PICK2 : AT_PICK2 + SLOTS]
    one = dots[:SLOTS] / divisor + pick * remain
    two = dots[AT_SECOND : AT_SECOND + SLOTS] / divisor + pick2 * remain
    dg_ref[step : step + 1, :] = bidiag
    n = gr_ref.shape[1] // LANES
    v_ref[step : step + 1, :] = jnp.where(gr_ref[...] == step, 1.0, c_ref[...] / wide(divisor, n))
    at_slot = lax.broadcasted_iota(jnp.int32, (SLOTS, LANES), 0) == step
    image = jnp.zeros((own_ref.shape[0], LANES), F32)
    first = second = pick_y = pick_u = jnp.zeros((SLOTS, LANES), F32)
    squares = lead = jnp.zeros((1, LANES), F32)
    half = cols // 2
    for begin in range(0, cols, LANES):
        ts = slice(begin, begin + LANES)
        y_t, u_t, piv_t, gc_t = y_ref[:, ts], u_ref[:, ts], pivot[:, ts], gc_ref[:, ts]
        y = factor * (summed[:, ts] / divisor + piv_t * remain - total(one * y_t + two * u_t))
        y = jnp.where(gc_t > step, y, 0.0)
        r = piv_t - total(pick * y_t + pick2 * u_t) - y
        r = jnp.where(gc_t > step, r, 0.0)
        y_ref[step : step + 1, ts] = y
        r_ref[:, ts] = r
        y_t = jnp.where(at_slot, y, y_t)
        first, second, squares = first + y_t * r, second + u_t * r, squares + r * r
        if begin % half == 0:
            hit = gc_t == step + 1
            lead = lead + jnp.where(hit, r, 0.0)
            pick_y = pick_y + jnp.where(hit, y_t, 0.0)
            pick_u = pick_u + jnp.where(hit, u_t, 0.0)
        block = own_ref[:, ts] if begin < half else oth_ref[:, begin - half : begin - half + LANES]
        image = image + block * r
    msg_ref[...] = jnp.concatenate(
        [gather_lanes(image), dots_row(first, second, squares, lead, pick_y, pick_u)], axis=1
    )


def call(kernel, name, ins, outs):
    return pl.pallas_call(
        kernel,
        name=name,
        out_shape=[pltpu.VMEM(s, F32) for s in outs],
        in_specs=[VMEM] * len(ins),
        out_specs=[VMEM] * len(outs),
        compiler_params=pltpu.CompilerParams(vmem_limit_bytes=2 << 20),
    )(*(pltpu.with_memory_space_constraint(x, pltpu.VMEM) for x in ins))


def per_device(weights):
    batch_n, row_cycles, tile_len, col_cycles, _ = weights.shape
    rows, cols = row_cycles * tile_len, col_cycles * tile_len
    w = weights.reshape(batch_n, rows, cols)
    row_devices, col_devices = lax.axis_size("row"), lax.axis_size("col")
    row_place, col_place = lax.axis_index("row"), lax.axis_index("col")
    core, chip = col_place % 2, col_place // 2
    chips = col_devices // 2
    everyone = range(col_devices)
    swap = [(i, i ^ 1) for i in everyone]
    near = [(i, i ^ 2) for i in everyone]
    far = [(i, 2 * (chips - 1 - i // 2) + i % 2) for i in everyone]

    col_ids = jnp.arange(cols, dtype=jnp.int32)

    def global_cols(place):
        return col_ids // tile_len * (col_devices * tile_len) + place * tile_len + col_ids % tile_len

    gcol = global_cols(col_place)
    gc = jnp.concatenate([gcol, global_cols(col_place ^ 1)])[None]
    grow = row_place * tile_len + jnp.arange(rows, dtype=jnp.int32)
    gr = grow[None]

    own = jnp.where(core == 0, w[0], w[1])
    oth = lax.ppermute(jnp.where(core == 0, w[1], w[0]), "col", swap)

    both = 2 * cols
    piece = TOTAL * both // row_devices
    flags = [jnp.full((1, LANES), place, jnp.int32) for place in (core, chip)]
    (slab,) = call(open_kernel, "open", (*flags, own, oth), ((SLOTS, rows),))
    slab = slab + lax.ppermute(slab, "col", [(0, 2), (1, 3)])
    first_cols = slab + lax.ppermute(slab, "col", [(0, 6), (1, 7), (2, 4), (3, 5)])

    vec_r, vec_c, flag = (SLOTS, rows), (SLOTS, both), (SLOTS, LANES)
    msg = (row_devices, 1, both + LANES)
    msg_first = (row_devices, 1, 2 * both + LANES + piece)
    msg_second = (row_devices, 1, both + LANES + piece)
    out = call(
        first_kernel,
        "first",
        (gr, first_cols, own, oth),
        (msg_first, (1, rows), vec_r, vec_r, vec_c, vec_c, flag, flag),
    )
    message, column, v, x, y, u, dg, sd = out
    for step in range(TOTAL):
        recv = lax.all_to_all(message, "row", split_axis=0, concat_axis=0, tiled=True)
        lead_in = (recv, column, gr, gc)
        state = (own, oth, u, v, y, dg)
        outs = ((1, rows + LANES), (1, both), vec_r, vec_c, flag)
        kernel = functools.partial(row_kernel, step)
        ins = lead_in + state
        if step == 0:
            message, r, v, y, dg, share = call(kernel, "row_step", ins, outs + ((1, piece),))
        elif step == 1:
            message, r, v, y, dg, pivots = call(kernel, "row_step", ins, outs + (vec_c,))
        else:
            message, r, v, y, dg = call(kernel, "row_step", ins + (pivots,), outs)
        part = message + lax.ppermute(message, "col", near)
        rest = lax.ppermute(part, "col", far)
        if step + 1 < TOTAL:
            ins = (part, rest, r, gr, gc, first_cols, own, oth, v, x, u, sd)
            if step == 0:
                ins += (share,)
            outs = (msg if step else msg_second, (1, rows), vec_r, vec_c, flag)
            kernel = functools.partial(column_kernel, step + 1)
            message, column, x, u, sd = call(kernel, "column_step", ins, outs)
    ins = (part, rest, r, gr, gc, first_cols, v, y, dg, x, u, sd)
    packed = (2 * SLOTS, rows + cols + LANES)
    mine, theirs, _, _, _ = call(last_kernel, "last", ins, (packed, packed, vec_r, vec_c, flag))
    theirs = lax.ppermute(theirs, "col", swap)
    packs = jnp.stack(
        [jnp.where(core == 0, mine, theirs), jnp.where(core == 0, theirs, mine)]
    )
    change = jnp.einsum(
        "mpr,mpc->mrc",
        packs[:, :, :rows],
        packs[:, :, rows : rows + cols],
        precision=lax.Precision.HIGHEST,
    )
    inside = (grow[:, None] >= TOTAL) & (gcol[None, :] >= TOTAL)
    trailing = jnp.where(inside[None], w - change, 0.0).reshape(weights.shape)
    ends = packs[:, :, rows + cols]
    return trailing, ends[:, :TOTAL], ends[:, SLOTS : SLOTS + TOTAL]


def solution(mesh):
    placed = P(None, None, "row", None, "col")
    return jax.shard_map(
        per_device,
        mesh=mesh,
        in_specs=(placed,),
        out_specs=(placed, P(), P()),
        check_vma=False,
    )
```

```python
import functools

import jax
import jax.numpy as jnp
from jax import lax
from jax.experimental import pallas as pl
from jax.experimental.pallas import tpu as pltpu
from jax.sharding import PartitionSpec as P

TOTAL = 12
SLOTS = 16
LANES = 128
AT_SQUARES, AT_LEAD, AT_SECOND, AT_PICK, AT_PICK2 = 32, 33, 16, 64, 80
VMEM = pl.BlockSpec(memory_space=pltpu.VMEM)
F32 = jnp.float32


def spread(row):
    return jnp.transpose(jnp.broadcast_to(row, (LANES, LANES)))


def gather_lanes(rows):
    return jnp.sum(jnp.transpose(rows), axis=0, keepdims=True)


def total(x):
    return jnp.sum(x, axis=0, keepdims=True)


def wide(x, n):
    return jnp.concatenate([x] * n, axis=1)


def fold(x):
    return sum(x[:, at : at + LANES] for at in range(0, x.shape[1], LANES))


def dots_row(first, second, squares, lead, pick, pick2):
    at = lax.broadcasted_iota(jnp.int32, (SLOTS, LANES), 0)
    pair = jnp.where(at == 0, squares, jnp.where(at == 1, lead, 0.0))
    none = jnp.zeros((SLOTS, LANES), F32)
    return gather_lanes(jnp.concatenate([first, second, pair, none, pick, pick2, none, none], axis=0))


def reflect(dots):
    lead = dots[AT_LEAD : AT_LEAD + 1]
    length = jnp.sqrt(dots[AT_SQUARES : AT_SQUARES + 1])
    divisor = jnp.maximum(lead + length, 1.0)
    factor = (lead + length) / jnp.maximum(length, 1.0)
    return divisor, factor, 1.0 - lead / divisor, -length


def slot(ref, at):
    return ref.at[at : at + 1]


def tiles(ref):
    return [slice(at, at + LANES) for at in range(0, ref.shape[1], LANES)]


def finish_row_side(step, sums, r_ref, gr_ref, gc_ref, cols_ref, v_ref, x_ref, u_ref, sd_ref):
    rows = gr_ref.shape[1]
    dots = spread(sums[:, rows:])
    divisor, factor, remain, bidiag = reflect(dots)
    pick, pick2 = dots[AT_PICK : AT_PICK + SLOTS], dots[AT_PICK2 : AT_PICK2 + SLOTS]
    one = dots[:SLOTS] / divisor + pick * remain
    two = dots[AT_SECOND : AT_SECOND + SLOTS] / divisor + pick2 * remain
    n = rows // LANES
    col = cols_ref[step : step + 1]
    v, x = v_ref[...], x_ref[...]
    image = wide(factor, n) * (
        sums[:, :rows] / wide(divisor, n)
        + col * wide(remain, n)
        - total(wide(one, n) * v + wide(two, n) * x)
    )
    image = jnp.where(gr_ref[...] >= step, image, 0.0)
    column = col - total(wide(pick, n) * v + wide(pick2, n) * x) - image
    x_ref[step - 1 : step, :] = image
    sd_ref[step - 1 : step, :] = bidiag
    for ts in tiles(r_ref):
        u_ref[step - 1 : step, ts] = jnp.where(gc_ref[:, ts] == step, 1.0, r_ref[:, ts] / divisor)
    return jnp.where(gr_ref[...] >= step, column, 0.0)


def send_row(step, column, gr_ref, own_ref, oth_ref, v_ref, x_ref, msg_ref, c_ref, extra=None):
    rows = gr_ref.shape[1]
    c_ref[...] = column
    spread_c = jnp.transpose(jnp.broadcast_to(column, (LANES, rows)))
    parts = []
    for ref in (own_ref, oth_ref):
        for ts in tiles(ref):
            parts.append(total(ref[:, ts] * spread_c))
    hit = gr_ref[...] == step
    lead = fold(jnp.where(hit, column, 0.0))
    squares = fold(column * column)
    if v_ref is None:
        none = jnp.zeros((SLOTS, LANES), F32)
        parts.append(dots_row(none, none, squares, lead, none, none))
    else:
        v, x = v_ref[...], x_ref[...]
        parts.append(
            dots_row(
                fold(v * column),
                fold(x * column),
                squares,
                lead,
                fold(jnp.where(hit, v, 0.0)),
                fold(jnp.where(hit, x, 0.0)),
            )
        )
    if extra is not None:
        parts.append(extra)
    message = jnp.concatenate(parts, axis=1)
    for peer in range(msg_ref.shape[0]):
        msg_ref[peer] = message


def carry(before, after):
    for old, new in zip(before, after):
        new[...] = old[...]


def open_kernel(core_ref, chip_ref, own_ref, oth_ref, slab_ref):
    slab = jnp.where(core_ref[...] == 0, own_ref[:, :LANES], oth_ref[:, :LANES])
    slab = jnp.transpose(slab)[:SLOTS]
    n = slab.shape[1] // LANES
    slab_ref[...] = jnp.where(wide(chip_ref[...], n) == 0, slab, 0.0)


def first_kernel(
    s0_ref, s1_ref, s2_ref, s3_ref, gr_ref, gc_ref, own_ref, oth_ref, msg_ref, c_ref, cols_ref, *state
):
    cols_ref[...] = (s0_ref[...] + s1_ref[...]) + (s2_ref[...] + s3_ref[...])
    for ref in state:
        ref[...] = jnp.zeros_like(ref)
    half = own_ref.shape[1]
    row = jnp.concatenate([own_ref[0:1], oth_ref[0:1]], axis=1)
    base = 4 * half + LANES
    send_row(
        0, cols_ref[0:1], gr_ref, own_ref, oth_ref, None, None, msg_ref.at[:, :, :base], c_ref, row
    )
    piece = msg_ref.shape[2] - base
    for peer in range(msg_ref.shape[0]):
        for at in range(0, piece, LANES):
            row, begin = divmod(peer * piece + at, 2 * half)
            ref = own_ref if begin < half else oth_ref
            begin %= half
            msg_ref[peer, :, base + at : base + at + LANES] = ref[row : row + 1, begin : begin + LANES]


def column_kernel(
    step, p0_ref, p1_ref, p2_ref, p3_ref, r_ref, gr_ref, gc_ref, cols_ref, own_ref, oth_ref, v_ref,
    x_in, u_in, sd_in, *refs,
):
    piece_ref = refs[0] if step == 1 else None
    msg_ref, c_ref, x_ref, u_ref, sd_ref = refs[-5:]
    carry((x_in, u_in, sd_in), (x_ref, u_ref, sd_ref))
    sums = (p0_ref[...] + p1_ref[...]) + (p2_ref[...] + p3_ref[...])
    column = finish_row_side(
        step, sums, r_ref, gr_ref, gc_ref, cols_ref, v_ref, x_ref, u_ref, sd_ref
    )
    extra = None if piece_ref is None else piece_ref[...]
    send_row(step, column, gr_ref, own_ref, oth_ref, v_ref, x_ref, msg_ref, c_ref, extra)


def last_kernel(
    p0_ref, p1_ref, p2_ref, p3_ref, r_ref, gr_ref, gc_ref, cols_ref, v_ref, y_ref, dg_ref,
    x_in, u_in, sd_in, own_ref, oth_ref, x_ref, u_ref, sd_ref,
):
    carry((x_in, u_in, sd_in), (x_ref, u_ref, sd_ref))
    sums = (p0_ref[...] + p1_ref[...]) + (p2_ref[...] + p3_ref[...])
    finish_row_side(TOTAL, sums, r_ref, gr_ref, gc_ref, cols_ref, v_ref, x_ref, u_ref, sd_ref)
    rows, half = gr_ref.shape[1], gc_ref.shape[1] // 2
    for ref, begin in ((own_ref, 0), (oth_ref, half)):
        ref[:SLOTS, :rows] = v_ref[...]
        ref[SLOTS:, :rows] = x_ref[...]
        ref[:SLOTS, rows : rows + half] = y_ref[:, begin : begin + half]
        ref[SLOTS:, rows : rows + half] = u_ref[:, begin : begin + half]
        ref[:SLOTS, rows + half :] = dg_ref[...]
        ref[SLOTS:, rows + half :] = sd_ref[...]


def row_kernel(
    step, recv_ref, c_ref, gr_ref, gc_ref, *refs,
):
    own_ref, oth_ref, u_ref, v_in, y_in, dg_in = refs[:6]
    if step == 0:
        msg_ref, r_ref, v_ref, y_ref, dg_ref, piece_ref = refs[6:]
    elif step == 1:
        msg_ref, r_ref, v_ref, y_ref, dg_ref, piv_ref = refs[6:]
    else:
        piv_ref, msg_ref, r_ref, v_ref, y_ref, dg_ref = refs[6:]
    carry((v_in, y_in, dg_in), (v_ref, y_ref, dg_ref))
    cols = gc_ref.shape[1]
    base = cols + LANES
    summed = recv_ref[0, :, :base]
    for peer in range(1, recv_ref.shape[0]):
        summed = summed + recv_ref[peer, :, :base]
    if step == 0:
        pivot = recv_ref[0, :, base : base + cols]
        piece_ref[...] = recv_ref[0, :, base + cols :]
    else:
        if step == 1:
            piece = recv_ref.shape[2] - base
            piv_ref[TOTAL:, :] = jnp.zeros((SLOTS - TOTAL, cols), F32)
            for peer in range(recv_ref.shape[0]):
                for at in range(0, piece, LANES):
                    row, begin = divmod(peer * piece + at, cols)
                    part = recv_ref[peer, :, base + at : base + at + LANES]
                    piv_ref[row : row + 1, begin : begin + LANES] = part
        pivot = piv_ref[step : step + 1]
    dots = spread(summed[:, cols:])
    divisor, factor, remain, bidiag = reflect(dots)
    pick, pick2 = dots[AT_PICK : AT_PICK + SLOTS], dots[AT_PICK2 : AT_PICK2 + SLOTS]
    one = dots[:SLOTS] / divisor + pick * remain
    two = dots[AT_SECOND : AT_SECOND + SLOTS] / divisor + pick2 * remain
    dg_ref[step : step + 1, :] = bidiag
    n = gr_ref.shape[1] // LANES
    v_ref[step : step + 1, :] = jnp.where(gr_ref[...] == step, 1.0, c_ref[...] / wide(divisor, n))
    at_slot = lax.broadcasted_iota(jnp.int32, (SLOTS, LANES), 0) == step
    image = jnp.zeros((own_ref.shape[0], LANES), F32)
    first = second = pick_y = pick_u = jnp.zeros((SLOTS, LANES), F32)
    squares = lead = jnp.zeros((1, LANES), F32)
    half = cols // 2
    for begin in range(0, cols, LANES):
        ts = slice(begin, begin + LANES)
        y_t, u_t, piv_t, gc_t = y_ref[:, ts], u_ref[:, ts], pivot[:, ts], gc_ref[:, ts]
        y = factor * (summed[:, ts] / divisor + piv_t * remain - total(one * y_t + two * u_t))
        y = jnp.where(gc_t > step, y, 0.0)
        r = piv_t - total(pick * y_t + pick2 * u_t) - y
        r = jnp.where(gc_t > step, r, 0.0)
        y_ref[step : step + 1, ts] = y
        r_ref[:, ts] = r
        y_t = jnp.where(at_slot, y, y_t)
        first, second, squares = first + y_t * r, second + u_t * r, squares + r * r
        if begin % half == 0:
            hit = gc_t == step + 1
            lead = lead + jnp.where(hit, r, 0.0)
            pick_y = pick_y + jnp.where(hit, y_t, 0.0)
            pick_u = pick_u + jnp.where(hit, u_t, 0.0)
        block = own_ref[:, ts] if begin < half else oth_ref[:, begin - half : begin - half + LANES]
        image = image + block * r
    msg_ref[...] = jnp.concatenate(
        [gather_lanes(image), dots_row(first, second, squares, lead, pick_y, pick_u)], axis=1
    )


def call(kernel, name, ins, outs):
    return pl.pallas_call(
        kernel,
        name=name,
        out_shape=[pltpu.VMEM(s, F32) for s in outs],
        in_specs=[VMEM] * len(ins),
        out_specs=[VMEM] * len(outs),
        compiler_params=pltpu.CompilerParams(vmem_limit_bytes=2 << 20),
    )(*(pltpu.with_memory_space_constraint(x, pltpu.VMEM) for x in ins))


def per_device(weights):
    batch_n, row_cycles, tile_len, col_cycles, _ = weights.shape
    rows, cols = row_cycles * tile_len, col_cycles * tile_len
    w = weights.reshape(batch_n, rows, cols)
    row_devices, col_devices = lax.axis_size("row"), lax.axis_size("col")
    row_place, col_place = lax.axis_index("row"), lax.axis_index("col")
    core, chip = col_place % 2, col_place // 2
    chips = col_devices // 2
    everyone = range(col_devices)
    swap = [(i, i ^ 1) for i in everyone]
    hops = [[(i, (i + 2 * hop) % col_devices) for i in everyone] for hop in (2, 1, chips - 1)]

    col_ids = jnp.arange(cols, dtype=jnp.int32)

    def global_cols(place):
        return col_ids // tile_len * (col_devices * tile_len) + place * tile_len + col_ids % tile_len

    gcol = global_cols(col_place)
    gc = jnp.concatenate([gcol, global_cols(col_place ^ 1)])[None]
    grow = row_place * tile_len + jnp.arange(rows, dtype=jnp.int32)
    gr = grow[None]

    own = jnp.where(core == 0, w[0], w[1])
    oth = lax.ppermute(jnp.where(core == 0, w[1], w[0]), "col", swap)

    both = 2 * cols
    piece = TOTAL * both // row_devices
    flags = [jnp.full((1, LANES), place, jnp.int32) for place in (core, chip)]
    (slab,) = call(open_kernel, "open", (*flags, own, oth), ((SLOTS, rows),))
    slabs = [slab] + [lax.ppermute(slab, "col", hop) for hop in hops]

    vec_r, vec_c, flag = (SLOTS, rows), (SLOTS, both), (SLOTS, LANES)
    msg = (row_devices, 1, both + LANES)
    msg_first = (row_devices, 1, 2 * both + LANES + piece)
    msg_second = (row_devices, 1, both + LANES + piece)
    out = call(
        first_kernel,
        "first",
        (*slabs, gr, gc, own, oth),
        (msg_first, (1, rows), vec_r, vec_r, vec_r, vec_c, vec_c, flag, flag),
    )
    message, column, first_cols, v, x, y, u, dg, sd = out
    for step in range(TOTAL):
        recv = lax.all_to_all(message, "row", split_axis=0, concat_axis=0, tiled=True)
        lead_in = (recv, column, gr, gc)
        state = (own, oth, u, v, y, dg)
        outs = ((1, rows + LANES), (1, both), vec_r, vec_c, flag)
        kernel = functools.partial(row_kernel, step)
        ins = lead_in + state
        if step == 0:
            message, r, v, y, dg, share = call(kernel, "row_step", ins, outs + ((1, piece),))
        elif step == 1:
            message, r, v, y, dg, pivots = call(kernel, "row_step", ins, outs + (vec_c,))
        else:
            message, r, v, y, dg = call(kernel, "row_step", ins + (pivots,), outs)
        parts = (message, *(lax.ppermute(message, "col", hop) for hop in hops))
        if step + 1 < TOTAL:
            ins = parts + (r, gr, gc, first_cols, own, oth, v, x, u, sd)
            if step == 0:
                ins += (share,)
            outs = (msg if step else msg_second, (1, rows), vec_r, vec_c, flag)
            kernel = functools.partial(column_kernel, step + 1)
            message, column, x, u, sd = call(kernel, "column_step", ins, outs)
    ins = parts + (r, gr, gc, first_cols, v, y, dg, x, u, sd)
    packed = (2 * SLOTS, rows + cols + LANES)
    mine, theirs, _, _, _ = call(last_kernel, "last", ins, (packed, packed, vec_r, vec_c, flag))
    theirs = lax.ppermute(theirs, "col", swap)
    packs = jnp.stack(
        [jnp.where(core == 0, mine, theirs), jnp.where(core == 0, theirs, mine)]
    )
    change = jnp.einsum(
        "mpr,mpc->mrc",
        packs[:, :, :rows],
        packs[:, :, rows : rows + cols],
        precision=lax.Precision.HIGHEST,
    )
    inside = (grow[:, None] >= TOTAL) & (gcol[None, :] >= TOTAL)
    trailing = jnp.where(inside[None], w - change, 0.0).reshape(weights.shape)
    ends = packs[:, :, rows + cols]
    return trailing, ends[:, :TOTAL], ends[:, SLOTS : SLOTS + TOTAL]


def solution(mesh):
    placed = P(None, None, "row", None, "col")
    return jax.shard_map(
        per_device,
        mesh=mesh,
        in_specs=(placed,),
        out_specs=(placed, P(), P()),
        check_vma=False,
    )
```

```python
import functools

import jax
import jax.numpy as jnp
from jax import lax
from jax.experimental import pallas as pl
from jax.experimental.pallas import tpu as pltpu
from jax.sharding import PartitionSpec as P

EXCHANGED = (0, 1, 3, 5, 7, 9)
TOTAL = 12
SLOTS = 16
LANES = 128
AT_SQUARES, AT_LEAD, AT_SECOND, AT_PICK, AT_PICK2 = 32, 33, 16, 64, 80
VMEM = pl.BlockSpec(memory_space=pltpu.VMEM)
F32 = jnp.float32


def spread(row):
    return jnp.transpose(jnp.broadcast_to(row, (LANES, LANES)))


def gather_lanes(rows):
    return jnp.sum(jnp.transpose(rows), axis=0, keepdims=True)


def total(x):
    return jnp.sum(x, axis=0, keepdims=True)


def wide(x, n):
    return jnp.concatenate([x] * n, axis=1)


def fold(x):
    return sum(x[:, at : at + LANES] for at in range(0, x.shape[1], LANES))


def dots_row(first, second, squares, lead, pick, pick2):
    at = lax.broadcasted_iota(jnp.int32, (SLOTS, LANES), 0)
    pair = jnp.where(at == 0, squares, jnp.where(at == 1, lead, 0.0))
    none = jnp.zeros((SLOTS, LANES), F32)
    return gather_lanes(jnp.concatenate([first, second, pair, none, pick, pick2, none, none], axis=0))


def reflect(dots):
    lead = dots[AT_LEAD : AT_LEAD + 1]
    length = jnp.sqrt(dots[AT_SQUARES : AT_SQUARES + 1])
    divisor = jnp.maximum(lead + length, 1.0)
    factor = (lead + length) / jnp.maximum(length, 1.0)
    return divisor, factor, 1.0 - lead / divisor, -length


def slot(ref, at):
    return ref.at[at : at + 1]


def tiles(ref):
    return [slice(at, at + LANES) for at in range(0, ref.shape[1], LANES)]


def finish_row_side(step, sums, r_ref, gr_ref, gc_ref, cols_ref, v_ref, x_ref, u_ref, sd_ref):
    rows = gr_ref.shape[1]
    dots = spread(sums[:, rows:])
    divisor, factor, remain, bidiag = reflect(dots)
    pick, pick2 = dots[AT_PICK : AT_PICK + SLOTS], dots[AT_PICK2 : AT_PICK2 + SLOTS]
    one = dots[:SLOTS] / divisor + pick * remain
    two = dots[AT_SECOND : AT_SECOND + SLOTS] / divisor + pick2 * remain
    n = rows // LANES
    col = cols_ref[step : step + 1]
    v, x = v_ref[...], x_ref[...]
    image = wide(factor, n) * (
        sums[:, :rows] / wide(divisor, n)
        + col * wide(remain, n)
        - total(wide(one, n) * v + wide(two, n) * x)
    )
    image = jnp.where(gr_ref[...] >= step, image, 0.0)
    column = col - total(wide(pick, n) * v + wide(pick2, n) * x) - image
    x_ref[step - 1 : step, :] = image
    sd_ref[step - 1 : step, :] = bidiag
    for ts in tiles(r_ref):
        u_ref[step - 1 : step, ts] = jnp.where(gc_ref[:, ts] == step, 1.0, r_ref[:, ts] / divisor)
    return jnp.where(gr_ref[...] >= step, column, 0.0)


def send_row(step, column, gr_ref, own_ref, oth_ref, v_ref, x_ref, msg_ref, c_ref, extra=None):
    rows = gr_ref.shape[1]
    c_ref[...] = column
    spread_c = jnp.transpose(jnp.broadcast_to(column, (LANES, rows)))
    parts = []
    for ref in (own_ref, oth_ref):
        for ts in tiles(ref):
            parts.append(total(ref[:, ts] * spread_c))
    hit = gr_ref[...] == step
    lead = fold(jnp.where(hit, column, 0.0))
    squares = fold(column * column)
    if v_ref is None:
        none = jnp.zeros((SLOTS, LANES), F32)
        parts.append(dots_row(none, none, squares, lead, none, none))
    else:
        v, x = v_ref[...], x_ref[...]
        parts.append(
            dots_row(
                fold(v * column),
                fold(x * column),
                squares,
                lead,
                fold(jnp.where(hit, v, 0.0)),
                fold(jnp.where(hit, x, 0.0)),
            )
        )
    if extra is not None:
        parts.append(extra)
    message = jnp.concatenate(parts, axis=1)
    for peer in range(msg_ref.shape[0]):
        msg_ref[peer] = message


def carry(before, after):
    for old, new in zip(before, after):
        new[...] = old[...]


def open_kernel(core_ref, chip_ref, own_ref, oth_ref, slab_ref):
    slab = jnp.where(core_ref[...] == 0, own_ref[:, :LANES], oth_ref[:, :LANES])
    slab = jnp.transpose(slab)[:SLOTS]
    n = slab.shape[1] // LANES
    slab_ref[...] = jnp.where(wide(chip_ref[...], n) == 0, slab, 0.0)


def first_kernel(
    s0_ref, s1_ref, s2_ref, s3_ref, gr_ref, gc_ref, own_ref, oth_ref, msg_ref, c_ref, cols_ref, *state
):
    cols_ref[...] = (s0_ref[...] + s1_ref[...]) + (s2_ref[...] + s3_ref[...])
    for ref in state:
        ref[...] = jnp.zeros_like(ref)
    half = own_ref.shape[1]
    row = jnp.concatenate([own_ref[0:1], oth_ref[0:1]], axis=1)
    base = 4 * half + LANES
    send_row(
        0, cols_ref[0:1], gr_ref, own_ref, oth_ref, None, None, msg_ref.at[:, :, :base], c_ref, row
    )
    piece = msg_ref.shape[2] - base
    for peer in range(msg_ref.shape[0]):
        for at in range(0, piece, LANES):
            row, begin = divmod(peer * piece + at, 2 * half)
            ref = own_ref if begin < half else oth_ref
            begin %= half
            msg_ref[peer, :, base + at : base + at + LANES] = ref[row : row + 1, begin : begin + LANES]


def joined(parts):
    if len(parts) == 1:
        (ref,) = parts
        return (ref[0] + ref[2]) + (ref[1] + ref[3])
    near = [ref[...] for ref in parts]
    return (near[0] + near[1]) + (near[2] + near[3])


def column_kernel(
    step, n, *refs
):
    parts, (r_ref, gr_ref, gc_ref, cols_ref, own_ref, oth_ref, v_ref, *refs) = refs[:n], refs[n:]
    x_in, u_in, sd_in, *refs = refs
    piece_ref = refs[0] if step == 1 else None
    msg_ref, c_ref, x_ref, u_ref, sd_ref = refs[-5:]
    carry((x_in, u_in, sd_in), (x_ref, u_ref, sd_ref))
    sums = joined(parts)
    column = finish_row_side(
        step, sums, r_ref, gr_ref, gc_ref, cols_ref, v_ref, x_ref, u_ref, sd_ref
    )
    extra = None if piece_ref is None else piece_ref[...]
    send_row(step, column, gr_ref, own_ref, oth_ref, v_ref, x_ref, msg_ref, c_ref, extra)


def last_kernel(
    n, *refs
):
    parts, (r_ref, gr_ref, gc_ref, cols_ref, v_ref, y_ref, dg_ref, *refs) = refs[:n], refs[n:]
    x_in, u_in, sd_in, own_ref, oth_ref, x_ref, u_ref, sd_ref = refs
    carry((x_in, u_in, sd_in), (x_ref, u_ref, sd_ref))
    sums = joined(parts)
    finish_row_side(TOTAL, sums, r_ref, gr_ref, gc_ref, cols_ref, v_ref, x_ref, u_ref, sd_ref)
    rows, half = gr_ref.shape[1], gc_ref.shape[1] // 2
    for ref, begin in ((own_ref, 0), (oth_ref, half)):
        ref[:SLOTS, :rows] = v_ref[...]
        ref[SLOTS:, :rows] = x_ref[...]
        ref[:SLOTS, rows : rows + half] = y_ref[:, begin : begin + half]
        ref[SLOTS:, rows : rows + half] = u_ref[:, begin : begin + half]
        ref[:SLOTS, rows + half :] = dg_ref[...]
        ref[SLOTS:, rows + half :] = sd_ref[...]


def row_kernel(
    step, recv_ref, c_ref, gr_ref, gc_ref, *refs,
):
    own_ref, oth_ref, u_ref, v_in, y_in, dg_in = refs[:6]
    if step == 0:
        msg_ref, r_ref, v_ref, y_ref, dg_ref, piece_ref = refs[6:]
    elif step == 1:
        msg_ref, r_ref, v_ref, y_ref, dg_ref, piv_ref = refs[6:]
    else:
        piv_ref, msg_ref, r_ref, v_ref, y_ref, dg_ref = refs[6:]
    carry((v_in, y_in, dg_in), (v_ref, y_ref, dg_ref))
    cols = gc_ref.shape[1]
    base = cols + LANES
    summed = recv_ref[0, :, :base]
    for peer in range(1, recv_ref.shape[0]):
        summed = summed + recv_ref[peer, :, :base]
    if step == 0:
        pivot = recv_ref[0, :, base : base + cols]
        piece_ref[...] = recv_ref[0, :, base + cols :]
    else:
        if step == 1:
            piece = recv_ref.shape[2] - base
            piv_ref[TOTAL:, :] = jnp.zeros((SLOTS - TOTAL, cols), F32)
            for peer in range(recv_ref.shape[0]):
                for at in range(0, piece, LANES):
                    row, begin = divmod(peer * piece + at, cols)
                    part = recv_ref[peer, :, base + at : base + at + LANES]
                    piv_ref[row : row + 1, begin : begin + LANES] = part
        pivot = piv_ref[step : step + 1]
    dots = spread(summed[:, cols:])
    divisor, factor, remain, bidiag = reflect(dots)
    pick, pick2 = dots[AT_PICK : AT_PICK + SLOTS], dots[AT_PICK2 : AT_PICK2 + SLOTS]
    one = dots[:SLOTS] / divisor + pick * remain
    two = dots[AT_SECOND : AT_SECOND + SLOTS] / divisor + pick2 * remain
    dg_ref[step : step + 1, :] = bidiag
    n = gr_ref.shape[1] // LANES
    v_ref[step : step + 1, :] = jnp.where(gr_ref[...] == step, 1.0, c_ref[...] / wide(divisor, n))
    at_slot = lax.broadcasted_iota(jnp.int32, (SLOTS, LANES), 0) == step
    image = jnp.zeros((own_ref.shape[0], LANES), F32)
    first = second = pick_y = pick_u = jnp.zeros((SLOTS, LANES), F32)
    squares = lead = jnp.zeros((1, LANES), F32)
    half = cols // 2
    for begin in range(0, cols, LANES):
        ts = slice(begin, begin + LANES)
        y_t, u_t, piv_t, gc_t = y_ref[:, ts], u_ref[:, ts], pivot[:, ts], gc_ref[:, ts]
        y = factor * (summed[:, ts] / divisor + piv_t * remain - total(one * y_t + two * u_t))
        y = jnp.where(gc_t > step, y, 0.0)
        r = piv_t - total(pick * y_t + pick2 * u_t) - y
        r = jnp.where(gc_t > step, r, 0.0)
        y_ref[step : step + 1, ts] = y
        r_ref[:, ts] = r
        y_t = jnp.where(at_slot, y, y_t)
        first, second, squares = first + y_t * r, second + u_t * r, squares + r * r
        if begin % half == 0:
            hit = gc_t == step + 1
            lead = lead + jnp.where(hit, r, 0.0)
            pick_y = pick_y + jnp.where(hit, y_t, 0.0)
            pick_u = pick_u + jnp.where(hit, u_t, 0.0)
        block = own_ref[:, ts] if begin < half else oth_ref[:, begin - half : begin - half + LANES]
        image = image + block * r
    message = jnp.concatenate(
        [gather_lanes(image), dots_row(first, second, squares, lead, pick_y, pick_u)], axis=1
    )
    msg_ref[...] = jnp.broadcast_to(message, msg_ref.shape)


def call(kernel, name, ins, outs):
    return pl.pallas_call(
        kernel,
        name=name,
        out_shape=[pltpu.VMEM(s, F32) for s in outs],
        in_specs=[VMEM] * len(ins),
        out_specs=[VMEM] * len(outs),
        compiler_params=pltpu.CompilerParams(vmem_limit_bytes=2 << 20),
    )(*(pltpu.with_memory_space_constraint(x, pltpu.VMEM) for x in ins))


def close_kernel(w_ref, pack_ref, row_ref, col_ref, out_ref):
    rows, tile_len = pl.num_programs(1) * w_ref.shape[2], w_ref.shape[4]
    below = row_ref[...] >= TOTAL
    at = pl.ds(pl.multiple_of(pl.program_id(1) * LANES, LANES), LANES)
    left = pack_ref[0, :, at]
    for t in range(w_ref.shape[3]):
        cols = slice(rows + t * tile_len, rows + (t + 1) * tile_len)
        change = lax.dot_general(
            left,
            pack_ref[0, :, cols],
            (((0,), (0,)), ((), ())),
            precision=lax.Precision.HIGHEST,
            preferred_element_type=F32,
        )
        inside = below & (col_ref[:, t * tile_len : (t + 1) * tile_len] >= TOTAL)
        out_ref[0, 0, :, t, :] = jnp.where(inside, w_ref[0, 0, :, t, :] - change, 0.0)


def close(weights, packs, row_at, col_at):
    batch_n, _, rows, tiles_n, tile_len = weights.shape
    part = pl.BlockSpec((1, 1, LANES, tiles_n, tile_len), lambda m, i: (m, 0, i, 0, 0))
    return pl.pallas_call(
        close_kernel,
        name="close",
        grid=(batch_n, rows // LANES),
        out_shape=jax.ShapeDtypeStruct(weights.shape, F32),
        in_specs=[
            part,
            pl.BlockSpec((1, *packs.shape[1:]), lambda m, i: (m, 0, 0)),
            pl.BlockSpec((LANES, 1), lambda m, i: (i, 0)),
            pl.BlockSpec(col_at.shape, lambda m, i: (0, 0)),
        ],
        out_specs=part,
        compiler_params=pltpu.CompilerParams(vmem_limit_bytes=8 << 20),
    )(weights, packs, row_at, col_at)


def per_device(weights):
    batch_n, row_cycles, tile_len, col_cycles, _ = weights.shape
    rows, cols = row_cycles * tile_len, col_cycles * tile_len
    w = weights.reshape(batch_n, rows, cols)
    row_devices, col_devices = lax.axis_size("row"), lax.axis_size("col")
    row_place, col_place = lax.axis_index("row"), lax.axis_index("col")
    core, chip = col_place % 2, col_place // 2
    chips = col_devices // 2
    everyone = range(col_devices)
    swap = [(i, i ^ 1) for i in everyone]
    hops = [[(i, (i + 2 * hop) % col_devices) for i in everyone] for hop in (2, 1, chips - 1)]

    chain = [[2 * x + side for x in range(chips)] for side in range(2)]
    col_ids = jnp.arange(cols, dtype=jnp.int32)

    def global_cols(place):
        return col_ids // tile_len * (col_devices * tile_len) + place * tile_len + col_ids % tile_len

    gcol = global_cols(col_place)
    gc = jnp.concatenate([gcol, global_cols(col_place ^ 1)])[None]
    grow = row_place * tile_len + jnp.arange(rows, dtype=jnp.int32)
    gr = grow[None]

    own = jnp.where(core == 0, w[0], w[1])
    oth = lax.ppermute(jnp.where(core == 0, w[1], w[0]), "col", swap)

    both = 2 * cols
    piece = TOTAL * both // row_devices
    flags = [jnp.full((1, LANES), place, jnp.int32) for place in (core, chip)]
    (slab,) = call(open_kernel, "open", (*flags, own, oth), ((SLOTS, rows),))
    slabs = [slab] + [lax.ppermute(slab, "col", hop) for hop in hops]

    vec_r, vec_c, flag = (SLOTS, rows), (SLOTS, both), (SLOTS, LANES)
    msg = (row_devices, 1, both + LANES)
    msg_first = (row_devices, 1, 2 * both + LANES + piece)
    msg_second = (row_devices, 1, both + LANES + piece)
    out = call(
        first_kernel,
        "first",
        (*slabs, gr, gc, own, oth),
        (msg_first, (1, rows), vec_r, vec_r, vec_r, vec_c, vec_c, flag, flag),
    )
    message, column, first_cols, v, x, y, u, dg, sd = out
    for step in range(TOTAL):
        recv = lax.all_to_all(message, "row", split_axis=0, concat_axis=0, tiled=True)
        lead_in = (recv, column, gr, gc)
        state = (own, oth, u, v, y, dg)
        short = (1, rows + LANES)
        outs = ((chips, *short) if step in EXCHANGED else short, (1, both), vec_r, vec_c, flag)
        kernel = functools.partial(row_kernel, step)
        ins = lead_in + state
        if step == 0:
            message, r, v, y, dg, share = call(kernel, "row_step", ins, outs + ((1, piece),))
        elif step == 1:
            message, r, v, y, dg, pivots = call(kernel, "row_step", ins, outs + (vec_c,))
        else:
            message, r, v, y, dg = call(kernel, "row_step", ins + (pivots,), outs)
        if step in EXCHANGED:
            parts = (lax.all_to_all(message, "col", 0, 0, axis_index_groups=chain, tiled=True),)
        else:
            parts = (message, *(lax.ppermute(message, "col", hop) for hop in hops))
        if step + 1 < TOTAL:
            ins = parts + (r, gr, gc, first_cols, own, oth, v, x, u, sd)
            if step == 0:
                ins += (share,)
            outs = (msg if step else msg_second, (1, rows), vec_r, vec_c, flag)
            kernel = functools.partial(column_kernel, step + 1, len(parts))
            message, column, x, u, sd = call(kernel, "column_step", ins, outs)
    ins = parts + (r, gr, gc, first_cols, v, y, dg, x, u, sd)
    packed = (2 * SLOTS, rows + cols + LANES)
    mine, theirs, _, _, _ = call(functools.partial(last_kernel, len(parts)), "last", ins, (packed, packed, vec_r, vec_c, flag))
    theirs = lax.ppermute(theirs, "col", swap)
    packs = jnp.stack(
        [jnp.where(core == 0, mine, theirs), jnp.where(core == 0, theirs, mine)]
    )
    row_at = grow[:, None]
    trailing = close(weights, packs, row_at, gcol[None])
    ends = packs[:, :, rows + cols]
    return trailing, ends[:, :TOTAL], ends[:, SLOTS : SLOTS + TOTAL]


def solution(mesh):
    placed = P(None, None, "row", None, "col")
    return jax.shard_map(
        per_device,
        mesh=mesh,
        in_specs=(placed,),
        out_specs=(placed, P(), P()),
        check_vma=False,
    )
```

```python
import functools

import jax
import jax.numpy as jnp
from jax import lax
from jax.experimental import pallas as pl
from jax.experimental.pallas import tpu as pltpu
from jax.sharding import PartitionSpec as P

EXCHANGED = range(6)
TOTAL = 12
SLOTS = 16
LANES = 128
AT_SQUARES, AT_LEAD, AT_SECOND, AT_PICK, AT_PICK2 = 32, 33, 16, 64, 80
VMEM = pl.BlockSpec(memory_space=pltpu.VMEM)
F32 = jnp.float32


def spread(row):
    return jnp.transpose(jnp.broadcast_to(row, (LANES, LANES)))


def gather_lanes(rows):
    return jnp.sum(jnp.transpose(rows), axis=0, keepdims=True)


def total(x):
    return jnp.sum(x, axis=0, keepdims=True)


def wide(x, n):
    return jnp.concatenate([x] * n, axis=1)


def fold(x):
    return sum(x[:, at : at + LANES] for at in range(0, x.shape[1], LANES))


def dots_row(first, second, squares, lead, pick, pick2):
    at = lax.broadcasted_iota(jnp.int32, (SLOTS, LANES), 0)
    pair = jnp.where(at == 0, squares, jnp.where(at == 1, lead, 0.0))
    none = jnp.zeros((SLOTS, LANES), F32)
    return gather_lanes(jnp.concatenate([first, second, pair, none, pick, pick2, none, none], axis=0))


def reflect(dots):
    lead = dots[AT_LEAD : AT_LEAD + 1]
    length = jnp.sqrt(dots[AT_SQUARES : AT_SQUARES + 1])
    divisor = jnp.maximum(lead + length, 1.0)
    factor = (lead + length) / jnp.maximum(length, 1.0)
    return divisor, factor, 1.0 - lead / divisor, -length


def slot(ref, at):
    return ref.at[at : at + 1]


def tiles(ref):
    return [slice(at, at + LANES) for at in range(0, ref.shape[1], LANES)]


def finish_row_side(step, sums, r_ref, gr_ref, gc_ref, cols_ref, v_ref, x_ref, u_ref, sd_ref):
    rows = gr_ref.shape[1]
    dots = spread(sums[:, rows:])
    divisor, factor, remain, bidiag = reflect(dots)
    pick, pick2 = dots[AT_PICK : AT_PICK + SLOTS], dots[AT_PICK2 : AT_PICK2 + SLOTS]
    one = dots[:SLOTS] / divisor + pick * remain
    two = dots[AT_SECOND : AT_SECOND + SLOTS] / divisor + pick2 * remain
    n = rows // LANES
    col = cols_ref[step : step + 1]
    v, x = v_ref[...], x_ref[...]
    image = wide(factor, n) * (
        sums[:, :rows] / wide(divisor, n)
        + col * wide(remain, n)
        - total(wide(one, n) * v + wide(two, n) * x)
    )
    image = jnp.where(gr_ref[...] >= step, image, 0.0)
    column = col - total(wide(pick, n) * v + wide(pick2, n) * x) - image
    x_ref[step - 1 : step, :] = image
    sd_ref[step - 1 : step, :] = bidiag
    for ts in tiles(r_ref):
        u_ref[step - 1 : step, ts] = jnp.where(gc_ref[:, ts] == step, 1.0, r_ref[:, ts] / divisor)
    return jnp.where(gr_ref[...] >= step, column, 0.0)


def send_row(step, column, gr_ref, own_ref, oth_ref, v_ref, x_ref, msg_ref, c_ref, extra=None):
    rows = gr_ref.shape[1]
    c_ref[...] = column
    spread_c = jnp.transpose(jnp.broadcast_to(column, (LANES, rows)))
    parts = []
    for ref in (own_ref, oth_ref):
        for ts in tiles(ref):
            parts.append(total(ref[:, ts] * spread_c))
    hit = gr_ref[...] == step
    lead = fold(jnp.where(hit, column, 0.0))
    squares = fold(column * column)
    if v_ref is None:
        none = jnp.zeros((SLOTS, LANES), F32)
        parts.append(dots_row(none, none, squares, lead, none, none))
    else:
        v, x = v_ref[...], x_ref[...]
        parts.append(
            dots_row(
                fold(v * column),
                fold(x * column),
                squares,
                lead,
                fold(jnp.where(hit, v, 0.0)),
                fold(jnp.where(hit, x, 0.0)),
            )
        )
    if extra is not None:
        parts.append(extra)
    message = jnp.concatenate(parts, axis=1)
    for peer in range(msg_ref.shape[0]):
        msg_ref[peer] = message


def carry(before, after):
    for old, new in zip(before, after):
        new[...] = old[...]


def open_kernel(core_ref, chip_ref, own_ref, oth_ref, slab_ref):
    slab = jnp.where(core_ref[...] == 0, own_ref[:, :LANES], oth_ref[:, :LANES])
    slab = jnp.transpose(slab)[:SLOTS]
    n = slab.shape[1] // LANES
    slab_ref[...] = jnp.where(wide(chip_ref[...], n) == 0, slab, 0.0)


def first_kernel(
    s0_ref, s1_ref, s2_ref, s3_ref, gr_ref, gc_ref, own_ref, oth_ref, msg_ref, c_ref, cols_ref, *state
):
    cols_ref[...] = (s0_ref[...] + s1_ref[...]) + (s2_ref[...] + s3_ref[...])
    for ref in state:
        ref[...] = jnp.zeros_like(ref)
    half = own_ref.shape[1]
    row = jnp.concatenate([own_ref[0:1], oth_ref[0:1]], axis=1)
    base = 4 * half + LANES
    send_row(
        0, cols_ref[0:1], gr_ref, own_ref, oth_ref, None, None, msg_ref.at[:, :, :base], c_ref, row
    )
    piece = msg_ref.shape[2] - base
    for peer in range(msg_ref.shape[0]):
        for at in range(0, piece, LANES):
            row, begin = divmod(peer * piece + at, 2 * half)
            ref = own_ref if begin < half else oth_ref
            begin %= half
            msg_ref[peer, :, base + at : base + at + LANES] = ref[row : row + 1, begin : begin + LANES]


def joined(parts):
    if len(parts) == 1:
        (ref,) = parts
        return (ref[0] + ref[2]) + (ref[1] + ref[3])
    near = [ref[...] for ref in parts]
    return (near[0] + near[1]) + (near[2] + near[3])


def column_kernel(
    step, n, *refs
):
    parts, (r_ref, gr_ref, gc_ref, cols_ref, own_ref, oth_ref, v_ref, *refs) = refs[:n], refs[n:]
    x_in, u_in, sd_in, *refs = refs
    piece_ref = refs[0] if step == 1 else None
    msg_ref, c_ref, x_ref, u_ref, sd_ref = refs[-5:]
    carry((x_in, u_in, sd_in), (x_ref, u_ref, sd_ref))
    sums = joined(parts)
    column = finish_row_side(
        step, sums, r_ref, gr_ref, gc_ref, cols_ref, v_ref, x_ref, u_ref, sd_ref
    )
    extra = None if piece_ref is None else piece_ref[...]
    send_row(step, column, gr_ref, own_ref, oth_ref, v_ref, x_ref, msg_ref, c_ref, extra)


def last_kernel(
    n, *refs
):
    parts, (r_ref, gr_ref, gc_ref, cols_ref, v_ref, y_ref, dg_ref, *refs) = refs[:n], refs[n:]
    x_in, u_in, sd_in, own_ref, oth_ref, x_ref, u_ref, sd_ref = refs
    carry((x_in, u_in, sd_in), (x_ref, u_ref, sd_ref))
    sums = joined(parts)
    finish_row_side(TOTAL, sums, r_ref, gr_ref, gc_ref, cols_ref, v_ref, x_ref, u_ref, sd_ref)
    rows, half = gr_ref.shape[1], gc_ref.shape[1] // 2
    for ref, begin in ((own_ref, 0), (oth_ref, half)):
        ref[:SLOTS, :rows] = v_ref[...]
        ref[SLOTS:, :rows] = x_ref[...]
        ref[:SLOTS, rows : rows + half] = y_ref[:, begin : begin + half]
        ref[SLOTS:, rows : rows + half] = u_ref[:, begin : begin + half]
        ref[:SLOTS, rows + half :] = dg_ref[...]
        ref[SLOTS:, rows + half :] = sd_ref[...]


def row_kernel(
    step, recv_ref, c_ref, gr_ref, gc_ref, *refs,
):
    own_ref, oth_ref, u_ref, v_in, y_in, dg_in = refs[:6]
    if step == 0:
        msg_ref, r_ref, v_ref, y_ref, dg_ref, piece_ref = refs[6:]
    elif step == 1:
        msg_ref, r_ref, v_ref, y_ref, dg_ref, piv_ref = refs[6:]
    else:
        piv_ref, msg_ref, r_ref, v_ref, y_ref, dg_ref = refs[6:]
    carry((v_in, y_in, dg_in), (v_ref, y_ref, dg_ref))
    cols = gc_ref.shape[1]
    base = cols + LANES
    summed = recv_ref[0, :, :base]
    for peer in range(1, recv_ref.shape[0]):
        summed = summed + recv_ref[peer, :, :base]
    if step == 0:
        pivot = recv_ref[0, :, base : base + cols]
        piece_ref[...] = recv_ref[0, :, base + cols :]
    else:
        if step == 1:
            piece = recv_ref.shape[2] - base
            piv_ref[TOTAL:, :] = jnp.zeros((SLOTS - TOTAL, cols), F32)
            for peer in range(recv_ref.shape[0]):
                for at in range(0, piece, LANES):
                    row, begin = divmod(peer * piece + at, cols)
                    part = recv_ref[peer, :, base + at : base + at + LANES]
                    piv_ref[row : row + 1, begin : begin + LANES] = part
        pivot = piv_ref[step : step + 1]
    dots = spread(summed[:, cols:])
    divisor, factor, remain, bidiag = reflect(dots)
    pick, pick2 = dots[AT_PICK : AT_PICK + SLOTS], dots[AT_PICK2 : AT_PICK2 + SLOTS]
    one = dots[:SLOTS] / divisor + pick * remain
    two = dots[AT_SECOND : AT_SECOND + SLOTS] / divisor + pick2 * remain
    dg_ref[step : step + 1, :] = bidiag
    n = gr_ref.shape[1] // LANES
    v_ref[step : step + 1, :] = jnp.where(gr_ref[...] == step, 1.0, c_ref[...] / wide(divisor, n))
    at_slot = lax.broadcasted_iota(jnp.int32, (SLOTS, LANES), 0) == step
    image = jnp.zeros((own_ref.shape[0], LANES), F32)
    first = second = pick_y = pick_u = jnp.zeros((SLOTS, LANES), F32)
    squares = lead = jnp.zeros((1, LANES), F32)
    half = cols // 2
    for begin in range(0, cols, LANES):
        ts = slice(begin, begin + LANES)
        y_t, u_t, piv_t, gc_t = y_ref[:, ts], u_ref[:, ts], pivot[:, ts], gc_ref[:, ts]
        y = factor * (summed[:, ts] / divisor + piv_t * remain - total(one * y_t + two * u_t))
        y = jnp.where(gc_t > step, y, 0.0)
        r = piv_t - total(pick * y_t + pick2 * u_t) - y
        r = jnp.where(gc_t > step, r, 0.0)
        y_ref[step : step + 1, ts] = y
        r_ref[:, ts] = r
        y_t = jnp.where(at_slot, y, y_t)
        first, second, squares = first + y_t * r, second + u_t * r, squares + r * r
        if begin % half == 0:
            hit = gc_t == step + 1
            lead = lead + jnp.where(hit, r, 0.0)
            pick_y = pick_y + jnp.where(hit, y_t, 0.0)
            pick_u = pick_u + jnp.where(hit, u_t, 0.0)
        block = own_ref[:, ts] if begin < half else oth_ref[:, begin - half : begin - half + LANES]
        image = image + block * r
    message = jnp.concatenate(
        [gather_lanes(image), dots_row(first, second, squares, lead, pick_y, pick_u)], axis=1
    )
    msg_ref[...] = jnp.broadcast_to(message, msg_ref.shape)


def call(kernel, name, ins, outs):
    return pl.pallas_call(
        kernel,
        name=name,
        out_shape=[pltpu.VMEM(s, F32) for s in outs],
        in_specs=[VMEM] * len(ins),
        out_specs=[VMEM] * len(outs),
        compiler_params=pltpu.CompilerParams(vmem_limit_bytes=2 << 20),
    )(*(pltpu.with_memory_space_constraint(x, pltpu.VMEM) for x in ins))


def close_kernel(w_ref, pack_ref, row_ref, col_ref, out_ref):
    rows, tile_len = pl.num_programs(1) * w_ref.shape[2], w_ref.shape[4]
    below = row_ref[...] >= TOTAL
    at = pl.ds(pl.multiple_of(pl.program_id(1) * LANES, LANES), LANES)
    left = pack_ref[0, :, at]
    for t in range(w_ref.shape[3]):
        cols = slice(rows + t * tile_len, rows + (t + 1) * tile_len)
        change = lax.dot_general(
            left,
            pack_ref[0, :, cols],
            (((0,), (0,)), ((), ())),
            precision=lax.Precision.HIGHEST,
            preferred_element_type=F32,
        )
        inside = below & (col_ref[:, t * tile_len : (t + 1) * tile_len] >= TOTAL)
        out_ref[0, 0, :, t, :] = jnp.where(inside, w_ref[0, 0, :, t, :] - change, 0.0)


def close(weights, packs, row_at, col_at):
    batch_n, _, rows, tiles_n, tile_len = weights.shape
    part = pl.BlockSpec((1, 1, LANES, tiles_n, tile_len), lambda m, i: (m, 0, i, 0, 0))
    return pl.pallas_call(
        close_kernel,
        name="close",
        grid=(batch_n, rows // LANES),
        out_shape=jax.ShapeDtypeStruct(weights.shape, F32),
        in_specs=[
            part,
            pl.BlockSpec((1, *packs.shape[1:]), lambda m, i: (m, 0, 0)),
            pl.BlockSpec((LANES, 1), lambda m, i: (i, 0)),
            pl.BlockSpec(col_at.shape, lambda m, i: (0, 0)),
        ],
        out_specs=part,
        compiler_params=pltpu.CompilerParams(vmem_limit_bytes=8 << 20),
    )(weights, packs, row_at, col_at)


def per_device(weights):
    batch_n, row_cycles, tile_len, col_cycles, _ = weights.shape
    rows, cols = row_cycles * tile_len, col_cycles * tile_len
    w = weights.reshape(batch_n, rows, cols)
    row_devices, col_devices = lax.axis_size("row"), lax.axis_size("col")
    row_place, col_place = lax.axis_index("row"), lax.axis_index("col")
    core, chip = col_place % 2, col_place // 2
    chips = col_devices // 2
    everyone = range(col_devices)
    swap = [(i, i ^ 1) for i in everyone]
    hops = [[(i, (i + 2 * hop) % col_devices) for i in everyone] for hop in (2, 1, chips - 1)]

    chain = [[2 * x + side for x in range(chips)] for side in range(2)]
    col_ids = jnp.arange(cols, dtype=jnp.int32)

    def global_cols(place):
        return col_ids // tile_len * (col_devices * tile_len) + place * tile_len + col_ids % tile_len

    gcol = global_cols(col_place)
    gc = jnp.concatenate([gcol, global_cols(col_place ^ 1)])[None]
    grow = row_place * tile_len + jnp.arange(rows, dtype=jnp.int32)
    gr = grow[None]

    own = jnp.where(core == 0, w[0], w[1])
    oth = lax.ppermute(jnp.where(core == 0, w[1], w[0]), "col", swap)

    both = 2 * cols
    piece = TOTAL * both // row_devices
    flags = [jnp.full((1, LANES), place, jnp.int32) for place in (core, chip)]
    (slab,) = call(open_kernel, "open", (*flags, own, oth), ((SLOTS, rows),))
    slabs = [slab] + [lax.ppermute(slab, "col", hop) for hop in hops]

    vec_r, vec_c, flag = (SLOTS, rows), (SLOTS, both), (SLOTS, LANES)
    msg = (row_devices, 1, both + LANES)
    msg_first = (row_devices, 1, 2 * both + LANES + piece)
    msg_second = (row_devices, 1, both + LANES + piece)
    out = call(
        first_kernel,
        "first",
        (*slabs, gr, gc, own, oth),
        (msg_first, (1, rows), vec_r, vec_r, vec_r, vec_c, vec_c, flag, flag),
    )
    message, column, first_cols, v, x, y, u, dg, sd = out
    for step in range(TOTAL):
        recv = lax.all_to_all(message, "row", split_axis=0, concat_axis=0, tiled=True)
        lead_in = (recv, column, gr, gc)
        state = (own, oth, u, v, y, dg)
        short = (1, rows + LANES)
        outs = ((chips, *short) if step in EXCHANGED else short, (1, both), vec_r, vec_c, flag)
        kernel = functools.partial(row_kernel, step)
        ins = lead_in + state
        if step == 0:
            message, r, v, y, dg, share = call(kernel, "row_step", ins, outs + ((1, piece),))
        elif step == 1:
            message, r, v, y, dg, pivots = call(kernel, "row_step", ins, outs + (vec_c,))
        else:
            message, r, v, y, dg = call(kernel, "row_step", ins + (pivots,), outs)
        if step in EXCHANGED:
            parts = (lax.all_to_all(message, "col", 0, 0, axis_index_groups=chain, tiled=True),)
        else:
            parts = (message, *(lax.ppermute(message, "col", hop) for hop in hops))
        if step + 1 < TOTAL:
            ins = parts + (r, gr, gc, first_cols, own, oth, v, x, u, sd)
            if step == 0:
                ins += (share,)
            outs = (msg if step else msg_second, (1, rows), vec_r, vec_c, flag)
            kernel = functools.partial(column_kernel, step + 1, len(parts))
            message, column, x, u, sd = call(kernel, "column_step", ins, outs)
    ins = parts + (r, gr, gc, first_cols, v, y, dg, x, u, sd)
    packed = (2 * SLOTS, rows + cols + LANES)
    mine, theirs, _, _, _ = call(functools.partial(last_kernel, len(parts)), "last", ins, (packed, packed, vec_r, vec_c, flag))
    theirs = lax.ppermute(theirs, "col", swap)
    packs = jnp.stack(
        [jnp.where(core == 0, mine, theirs), jnp.where(core == 0, theirs, mine)]
    )
    row_at = grow[:, None]
    trailing = close(weights, packs, row_at, gcol[None])
    ends = packs[:, :, rows + cols]
    return trailing, ends[:, :TOTAL], ends[:, SLOTS : SLOTS + TOTAL]


def solution(mesh):
    placed = P(None, None, "row", None, "col")
    return jax.shard_map(
        per_device,
        mesh=mesh,
        in_specs=(placed,),
        out_specs=(placed, P(), P()),
        check_vma=False,
    )
```

```python
import functools

import jax
import jax.numpy as jnp
from jax import lax
from jax.experimental import pallas as pl
from jax.experimental.pallas import tpu as pltpu
from jax.sharding import PartitionSpec as P

EXCHANGED = range(6, 12)
TOTAL = 12
SLOTS = 16
LANES = 128
AT_SQUARES, AT_LEAD, AT_SECOND, AT_PICK, AT_PICK2 = 32, 33, 16, 64, 80
VMEM = pl.BlockSpec(memory_space=pltpu.VMEM)
F32 = jnp.float32


def spread(row):
    return jnp.transpose(jnp.broadcast_to(row, (LANES, LANES)))


def gather_lanes(rows):
    return jnp.sum(jnp.transpose(rows), axis=0, keepdims=True)


def total(x):
    return jnp.sum(x, axis=0, keepdims=True)


def wide(x, n):
    return jnp.concatenate([x] * n, axis=1)


def fold(x):
    return sum(x[:, at : at + LANES] for at in range(0, x.shape[1], LANES))


def dots_row(first, second, squares, lead, pick, pick2):
    at = lax.broadcasted_iota(jnp.int32, (SLOTS, LANES), 0)
    pair = jnp.where(at == 0, squares, jnp.where(at == 1, lead, 0.0))
    none = jnp.zeros((SLOTS, LANES), F32)
    return gather_lanes(jnp.concatenate([first, second, pair, none, pick, pick2, none, none], axis=0))


def reflect(dots):
    lead = dots[AT_LEAD : AT_LEAD + 1]
    length = jnp.sqrt(dots[AT_SQUARES : AT_SQUARES + 1])
    divisor = jnp.maximum(lead + length, 1.0)
    factor = (lead + length) / jnp.maximum(length, 1.0)
    return divisor, factor, 1.0 - lead / divisor, -length


def slot(ref, at):
    return ref.at[at : at + 1]


def tiles(ref):
    return [slice(at, at + LANES) for at in range(0, ref.shape[1], LANES)]


def finish_row_side(step, sums, r_ref, gr_ref, gc_ref, cols_ref, v_ref, x_ref, u_ref, sd_ref):
    rows = gr_ref.shape[1]
    dots = spread(sums[:, rows:])
    divisor, factor, remain, bidiag = reflect(dots)
    pick, pick2 = dots[AT_PICK : AT_PICK + SLOTS], dots[AT_PICK2 : AT_PICK2 + SLOTS]
    one = dots[:SLOTS] / divisor + pick * remain
    two = dots[AT_SECOND : AT_SECOND + SLOTS] / divisor + pick2 * remain
    n = rows // LANES
    col = cols_ref[step : step + 1]
    v, x = v_ref[...], x_ref[...]
    image = wide(factor, n) * (
        sums[:, :rows] / wide(divisor, n)
        + col * wide(remain, n)
        - total(wide(one, n) * v + wide(two, n) * x)
    )
    image = jnp.where(gr_ref[...] >= step, image, 0.0)
    column = col - total(wide(pick, n) * v + wide(pick2, n) * x) - image
    x_ref[step - 1 : step, :] = image
    sd_ref[step - 1 : step, :] = bidiag
    for ts in tiles(r_ref):
        u_ref[step - 1 : step, ts] = jnp.where(gc_ref[:, ts] == step, 1.0, r_ref[:, ts] / divisor)
    return jnp.where(gr_ref[...] >= step, column, 0.0)


def send_row(step, column, gr_ref, own_ref, oth_ref, v_ref, x_ref, msg_ref, c_ref, extra=None):
    rows = gr_ref.shape[1]
    c_ref[...] = column
    spread_c = jnp.transpose(jnp.broadcast_to(column, (LANES, rows)))
    parts = []
    for ref in (own_ref, oth_ref):
        for ts in tiles(ref):
            parts.append(total(ref[:, ts] * spread_c))
    hit = gr_ref[...] == step
    lead = fold(jnp.where(hit, column, 0.0))
    squares = fold(column * column)
    if v_ref is None:
        none = jnp.zeros((SLOTS, LANES), F32)
        parts.append(dots_row(none, none, squares, lead, none, none))
    else:
        v, x = v_ref[...], x_ref[...]
        parts.append(
            dots_row(
                fold(v * column),
                fold(x * column),
                squares,
                lead,
                fold(jnp.where(hit, v, 0.0)),
                fold(jnp.where(hit, x, 0.0)),
            )
        )
    if extra is not None:
        parts.append(extra)
    message = jnp.concatenate(parts, axis=1)
    for peer in range(msg_ref.shape[0]):
        msg_ref[peer] = message


def carry(before, after):
    for old, new in zip(before, after):
        new[...] = old[...]


def open_kernel(core_ref, chip_ref, own_ref, oth_ref, slab_ref):
    slab = jnp.where(core_ref[...] == 0, own_ref[:, :LANES], oth_ref[:, :LANES])
    slab = jnp.transpose(slab)[:SLOTS]
    n = slab.shape[1] // LANES
    slab_ref[...] = jnp.where(wide(chip_ref[...], n) == 0, slab, 0.0)


def first_kernel(
    s0_ref, s1_ref, s2_ref, s3_ref, gr_ref, gc_ref, own_ref, oth_ref, msg_ref, c_ref, cols_ref, *state
):
    cols_ref[...] = (s0_ref[...] + s1_ref[...]) + (s2_ref[...] + s3_ref[...])
    for ref in state:
        ref[...] = jnp.zeros_like(ref)
    half = own_ref.shape[1]
    row = jnp.concatenate([own_ref[0:1], oth_ref[0:1]], axis=1)
    base = 4 * half + LANES
    send_row(
        0, cols_ref[0:1], gr_ref, own_ref, oth_ref, None, None, msg_ref.at[:, :, :base], c_ref, row
    )
    piece = msg_ref.shape[2] - base
    for peer in range(msg_ref.shape[0]):
        for at in range(0, piece, LANES):
            row, begin = divmod(peer * piece + at, 2 * half)
            ref = own_ref if begin < half else oth_ref
            begin %= half
            msg_ref[peer, :, base + at : base + at + LANES] = ref[row : row + 1, begin : begin + LANES]


def joined(parts):
    if len(parts) == 1:
        (ref,) = parts
        return (ref[0] + ref[2]) + (ref[1] + ref[3])
    near = [ref[...] for ref in parts]
    return (near[0] + near[1]) + (near[2] + near[3])


def column_kernel(
    step, n, *refs
):
    parts, (r_ref, gr_ref, gc_ref, cols_ref, own_ref, oth_ref, v_ref, *refs) = refs[:n], refs[n:]
    x_in, u_in, sd_in, *refs = refs
    piece_ref = refs[0] if step == 1 else None
    msg_ref, c_ref, x_ref, u_ref, sd_ref = refs[-5:]
    carry((x_in, u_in, sd_in), (x_ref, u_ref, sd_ref))
    sums = joined(parts)
    column = finish_row_side(
        step, sums, r_ref, gr_ref, gc_ref, cols_ref, v_ref, x_ref, u_ref, sd_ref
    )
    extra = None if piece_ref is None else piece_ref[...]
    send_row(step, column, gr_ref, own_ref, oth_ref, v_ref, x_ref, msg_ref, c_ref, extra)


def last_kernel(
    n, *refs
):
    parts, (r_ref, gr_ref, gc_ref, cols_ref, v_ref, y_ref, dg_ref, *refs) = refs[:n], refs[n:]
    x_in, u_in, sd_in, own_ref, oth_ref, x_ref, u_ref, sd_ref = refs
    carry((x_in, u_in, sd_in), (x_ref, u_ref, sd_ref))
    sums = joined(parts)
    finish_row_side(TOTAL, sums, r_ref, gr_ref, gc_ref, cols_ref, v_ref, x_ref, u_ref, sd_ref)
    rows, half = gr_ref.shape[1], gc_ref.shape[1] // 2
    for ref, begin in ((own_ref, 0), (oth_ref, half)):
        ref[:SLOTS, :rows] = v_ref[...]
        ref[SLOTS:, :rows] = x_ref[...]
        ref[:SLOTS, rows : rows + half] = y_ref[:, begin : begin + half]
        ref[SLOTS:, rows : rows + half] = u_ref[:, begin : begin + half]
        ref[:SLOTS, rows + half :] = dg_ref[...]
        ref[SLOTS:, rows + half :] = sd_ref[...]


def row_kernel(
    step, recv_ref, c_ref, gr_ref, gc_ref, *refs,
):
    own_ref, oth_ref, u_ref, v_in, y_in, dg_in = refs[:6]
    if step == 0:
        msg_ref, r_ref, v_ref, y_ref, dg_ref, piece_ref = refs[6:]
    elif step == 1:
        msg_ref, r_ref, v_ref, y_ref, dg_ref, piv_ref = refs[6:]
    else:
        piv_ref, msg_ref, r_ref, v_ref, y_ref, dg_ref = refs[6:]
    carry((v_in, y_in, dg_in), (v_ref, y_ref, dg_ref))
    cols = gc_ref.shape[1]
    base = cols + LANES
    summed = recv_ref[0, :, :base]
    for peer in range(1, recv_ref.shape[0]):
        summed = summed + recv_ref[peer, :, :base]
    if step == 0:
        pivot = recv_ref[0, :, base : base + cols]
        piece_ref[...] = recv_ref[0, :, base + cols :]
    else:
        if step == 1:
            piece = recv_ref.shape[2] - base
            piv_ref[TOTAL:, :] = jnp.zeros((SLOTS - TOTAL, cols), F32)
            for peer in range(recv_ref.shape[0]):
                for at in range(0, piece, LANES):
                    row, begin = divmod(peer * piece + at, cols)
                    part = recv_ref[peer, :, base + at : base + at + LANES]
                    piv_ref[row : row + 1, begin : begin + LANES] = part
        pivot = piv_ref[step : step + 1]
    dots = spread(summed[:, cols:])
    divisor, factor, remain, bidiag = reflect(dots)
    pick, pick2 = dots[AT_PICK : AT_PICK + SLOTS], dots[AT_PICK2 : AT_PICK2 + SLOTS]
    one = dots[:SLOTS] / divisor + pick * remain
    two = dots[AT_SECOND : AT_SECOND + SLOTS] / divisor + pick2 * remain
    dg_ref[step : step + 1, :] = bidiag
    n = gr_ref.shape[1] // LANES
    v_ref[step : step + 1, :] = jnp.where(gr_ref[...] == step, 1.0, c_ref[...] / wide(divisor, n))
    at_slot = lax.broadcasted_iota(jnp.int32, (SLOTS, LANES), 0) == step
    image = jnp.zeros((own_ref.shape[0], LANES), F32)
    first = second = pick_y = pick_u = jnp.zeros((SLOTS, LANES), F32)
    squares = lead = jnp.zeros((1, LANES), F32)
    half = cols // 2
    for begin in range(0, cols, LANES):
        ts = slice(begin, begin + LANES)
        y_t, u_t, piv_t, gc_t = y_ref[:, ts], u_ref[:, ts], pivot[:, ts], gc_ref[:, ts]
        y = factor * (summed[:, ts] / divisor + piv_t * remain - total(one * y_t + two * u_t))
        y = jnp.where(gc_t > step, y, 0.0)
        r = piv_t - total(pick * y_t + pick2 * u_t) - y
        r = jnp.where(gc_t > step, r, 0.0)
        y_ref[step : step + 1, ts] = y
        r_ref[:, ts] = r
        y_t = jnp.where(at_slot, y, y_t)
        first, second, squares = first + y_t * r, second + u_t * r, squares + r * r
        if begin % half == 0:
            hit = gc_t == step + 1
            lead = lead + jnp.where(hit, r, 0.0)
            pick_y = pick_y + jnp.where(hit, y_t, 0.0)
            pick_u = pick_u + jnp.where(hit, u_t, 0.0)
        block = own_ref[:, ts] if begin < half else oth_ref[:, begin - half : begin - half + LANES]
        image = image + block * r
    message = jnp.concatenate(
        [gather_lanes(image), dots_row(first, second, squares, lead, pick_y, pick_u)], axis=1
    )
    msg_ref[...] = jnp.broadcast_to(message, msg_ref.shape)


def call(kernel, name, ins, outs):
    return pl.pallas_call(
        kernel,
        name=name,
        out_shape=[pltpu.VMEM(s, F32) for s in outs],
        in_specs=[VMEM] * len(ins),
        out_specs=[VMEM] * len(outs),
        compiler_params=pltpu.CompilerParams(vmem_limit_bytes=2 << 20),
    )(*(pltpu.with_memory_space_constraint(x, pltpu.VMEM) for x in ins))


def close_kernel(w_ref, pack_ref, row_ref, col_ref, out_ref):
    rows, tile_len = pl.num_programs(1) * w_ref.shape[2], w_ref.shape[4]
    below = row_ref[...] >= TOTAL
    at = pl.ds(pl.multiple_of(pl.program_id(1) * LANES, LANES), LANES)
    left = pack_ref[0, :, at]
    for t in range(w_ref.shape[3]):
        cols = slice(rows + t * tile_len, rows + (t + 1) * tile_len)
        change = lax.dot_general(
            left,
            pack_ref[0, :, cols],
            (((0,), (0,)), ((), ())),
            precision=lax.Precision.HIGHEST,
            preferred_element_type=F32,
        )
        inside = below & (col_ref[:, t * tile_len : (t + 1) * tile_len] >= TOTAL)
        out_ref[0, 0, :, t, :] = jnp.where(inside, w_ref[0, 0, :, t, :] - change, 0.0)


def close(weights, packs, row_at, col_at):
    batch_n, _, rows, tiles_n, tile_len = weights.shape
    part = pl.BlockSpec((1, 1, LANES, tiles_n, tile_len), lambda m, i: (m, 0, i, 0, 0))
    return pl.pallas_call(
        close_kernel,
        name="close",
        grid=(batch_n, rows // LANES),
        out_shape=jax.ShapeDtypeStruct(weights.shape, F32),
        in_specs=[
            part,
            pl.BlockSpec((1, *packs.shape[1:]), lambda m, i: (m, 0, 0)),
            pl.BlockSpec((LANES, 1), lambda m, i: (i, 0)),
            pl.BlockSpec(col_at.shape, lambda m, i: (0, 0)),
        ],
        out_specs=part,
        compiler_params=pltpu.CompilerParams(vmem_limit_bytes=8 << 20),
    )(weights, packs, row_at, col_at)


def per_device(weights):
    batch_n, row_cycles, tile_len, col_cycles, _ = weights.shape
    rows, cols = row_cycles * tile_len, col_cycles * tile_len
    w = weights.reshape(batch_n, rows, cols)
    row_devices, col_devices = lax.axis_size("row"), lax.axis_size("col")
    row_place, col_place = lax.axis_index("row"), lax.axis_index("col")
    core, chip = col_place % 2, col_place // 2
    chips = col_devices // 2
    everyone = range(col_devices)
    swap = [(i, i ^ 1) for i in everyone]
    hops = [[(i, (i + 2 * hop) % col_devices) for i in everyone] for hop in (2, 1, chips - 1)]

    chain = [[2 * x + side for x in range(chips)] for side in range(2)]
    col_ids = jnp.arange(cols, dtype=jnp.int32)

    def global_cols(place):
        return col_ids // tile_len * (col_devices * tile_len) + place * tile_len + col_ids % tile_len

    gcol = global_cols(col_place)
    gc = jnp.concatenate([gcol, global_cols(col_place ^ 1)])[None]
    grow = row_place * tile_len + jnp.arange(rows, dtype=jnp.int32)
    gr = grow[None]

    own = jnp.where(core == 0, w[0], w[1])
    oth = lax.ppermute(jnp.where(core == 0, w[1], w[0]), "col", swap)

    both = 2 * cols
    piece = TOTAL * both // row_devices
    flags = [jnp.full((1, LANES), place, jnp.int32) for place in (core, chip)]
    (slab,) = call(open_kernel, "open", (*flags, own, oth), ((SLOTS, rows),))
    slabs = [slab] + [lax.ppermute(slab, "col", hop) for hop in hops]

    vec_r, vec_c, flag = (SLOTS, rows), (SLOTS, both), (SLOTS, LANES)
    msg = (row_devices, 1, both + LANES)
    msg_first = (row_devices, 1, 2 * both + LANES + piece)
    msg_second = (row_devices, 1, both + LANES + piece)
    out = call(
        first_kernel,
        "first",
        (*slabs, gr, gc, own, oth),
        (msg_first, (1, rows), vec_r, vec_r, vec_r, vec_c, vec_c, flag, flag),
    )
    message, column, first_cols, v, x, y, u, dg, sd = out
    for step in range(TOTAL):
        recv = lax.all_to_all(message, "row", split_axis=0, concat_axis=0, tiled=True)
        lead_in = (recv, column, gr, gc)
        state = (own, oth, u, v, y, dg)
        short = (1, rows + LANES)
        outs = ((chips, *short) if step in EXCHANGED else short, (1, both), vec_r, vec_c, flag)
        kernel = functools.partial(row_kernel, step)
        ins = lead_in + state
        if step == 0:
            message, r, v, y, dg, share = call(kernel, "row_step", ins, outs + ((1, piece),))
        elif step == 1:
            message, r, v, y, dg, pivots = call(kernel, "row_step", ins, outs + (vec_c,))
        else:
            message, r, v, y, dg = call(kernel, "row_step", ins + (pivots,), outs)
        if step in EXCHANGED:
            parts = (lax.all_to_all(message, "col", 0, 0, axis_index_groups=chain, tiled=True),)
        else:
            parts = (message, *(lax.ppermute(message, "col", hop) for hop in hops))
        if step + 1 < TOTAL:
            ins = parts + (r, gr, gc, first_cols, own, oth, v, x, u, sd)
            if step == 0:
                ins += (share,)
            outs = (msg if step else msg_second, (1, rows), vec_r, vec_c, flag)
            kernel = functools.partial(column_kernel, step + 1, len(parts))
            message, column, x, u, sd = call(kernel, "column_step", ins, outs)
    ins = parts + (r, gr, gc, first_cols, v, y, dg, x, u, sd)
    packed = (2 * SLOTS, rows + cols + LANES)
    mine, theirs, _, _, _ = call(functools.partial(last_kernel, len(parts)), "last", ins, (packed, packed, vec_r, vec_c, flag))
    theirs = lax.ppermute(theirs, "col", swap)
    packs = jnp.stack(
        [jnp.where(core == 0, mine, theirs), jnp.where(core == 0, theirs, mine)]
    )
    row_at = grow[:, None]
    trailing = close(weights, packs, row_at, gcol[None])
    ends = packs[:, :, rows + cols]
    return trailing, ends[:, :TOTAL], ends[:, SLOTS : SLOTS + TOTAL]


def solution(mesh):
    placed = P(None, None, "row", None, "col")
    return jax.shard_map(
        per_device,
        mesh=mesh,
        in_specs=(placed,),
        out_specs=(placed, P(), P()),
        check_vma=False,
    )
```
